512 devices in a mesh: row: 32 (over y, x, core), col: 16 (over z).
Axes of the slice: x: 4, y: 4, z: 16, core: 2. Of those that a mesh axis runs over, the one named last changes fastest.
Arguments:
- ensemble: float32 [65536, 1024], P(('row', 'col')), may hold values from -6 to 6
- obs_rows: int32 [2, 256], replicated, may hold values from 0 to 127
- owner: int32 [2], replicated, may hold values from 0 to 31
- obs_value: float32 [2, 256], replicated, may hold values from -8 to 8
- obs_var: float32 [2, 256], replicated, may hold values from 0.1 to 2
- taper_mask: int32 [2, 512, 2], P(None, ('row', 'col')), may hold values 0 or 1
Outputs:
- analysis: float32 [65536, 1024], P(('row', 'col'))
The draws below stay inside these ranges and needn't reach their ends.
Inputs may be any that keep to these rules, and one draw needn't show every extreme that they name: `obs_rows`: observation p of batch b lies on the device at col index p // (256 / 16) of group owner[b]; batches may repeat a group and an observation may repeat a row.
All inputs are finite; a program needn't handle non-finite values. No bound on the sum of `taper_mask` on one device may be relied on, other than what follows from the above.
Results may differ from the reference program's by a relative error of at most 0.00018.
Values sent between devices are 32-bit elements; how exact they have to be, the bound alone decides.
No kernel may reach another device: no remote copies, remote signals or barrier semaphores. Data moves between devices by JAX's collectives and lax.ppermute only.
A program may use at most 64 MiB of HBM per device.

```python
import math
import jax
import jax.numpy as jnp
from jax import lax

ROWS_DEV = 128
MEMBERS = 1024
OBS = 256
BATCHES = 2
BLK = 128
NSTATE = 65536
N_ROW = 32
N_COL = 16


def touch_ends(values, stream_key, smallest, largest):
    place = [jax.random.randint(jax.random.fold_in(stream_key, axis), (), 0, length) for axis, length in enumerate(values.shape)]
    longest = values.shape.index(max(values.shape))
    neighbour = place[:longest] + [(place[longest] + 1) % values.shape[longest]] + place[longest + 1:]
    return values.at[tuple(place)].set(smallest).at[tuple(neighbour)].set(largest)


def levels(key, shape, split, least, top_value):
    level = 1.0
    for position, parts in split:
        heights = jax.random.uniform(jax.random.fold_in(jax.random.fold_in(key, 6), position), (parts,), jnp.float32, least / len(split), top_value / len(split))
        level = level * jnp.repeat(jnp.exp(heights), shape[position] // parts).reshape((-1,) + (1,) * (len(shape) - 1 - position))
    return level


def noise(stream_key, shape, scale, limit, cuts=(), held_as=jnp.bfloat16):
    array = scale * jax.random.normal(stream_key, shape, jnp.float32)
    if cuts:
        array = array * levels(stream_key, shape, cuts, -0.22, 0.18)
    return jnp.clip(array, -limit, limit).astype(held_as)


def setup_inputs(seed: int = 0) -> dict:
    key_of = jax.random.split(jax.random.key(seed), 7)
    ensemble = noise(key_of[0], (NSTATE, MEMBERS), 1.0, 6.0, ((0, 512),), jnp.float32)
    obs_rows = touch_ends(jax.random.randint(key_of[1], (BATCHES, OBS), 0, ROWS_DEV), jax.random.fold_in(key_of[1], 1), 0, ROWS_DEV - 1).astype(jnp.int32)
    owner = jax.random.randint(key_of[2], (BATCHES,), 0, N_ROW).astype(jnp.int32)
    obs_value = noise(key_of[3], (BATCHES, OBS), 1.5, 8.0, (), jnp.float32)
    obs_var = jnp.clip(jnp.exp(jax.random.uniform(key_of[4], (BATCHES, OBS), jnp.float32, math.log(0.1), math.log(2.0))), 0.1, 2.0)
    taper_mask = touch_ends((jax.random.randint(key_of[5], (BATCHES, NSTATE // BLK, OBS // BLK), 0, 4) < 3).astype(jnp.int32), jax.random.fold_in(key_of[5], 1), 0, 1)
    return dict(ensemble=ensemble, obs_rows=obs_rows, owner=owner, obs_value=obs_value, obs_var=obs_var, taper_mask=taper_mask)


def invert_spd(cov):
    count = cov.shape[0]
    factor = jnp.linalg.cholesky(cov)
    ident = jnp.eye(count, dtype=cov.dtype)
    lower_inv = lax.linalg.triangular_solve(factor, ident, left_side=True, lower=True)
    return lax.linalg.triangular_solve(factor, lower_inv, left_side=True, lower=True, transpose_a=True)

def reference(ensemble, obs_rows, owner, obs_value, obs_var, taper_mask):
    total = ensemble.shape[0]
    members = ensemble.shape[1]
    count = obs_rows.shape[1]
    per_dev = count // N_COL
    local_len = total // 4
    positions = jnp.arange(total, dtype=jnp.int32)
    state = ensemble
    for batch in range(BATCHES):
        mean = jnp.mean(state, axis=1, keepdims=True)
        anom = state - mean
        column_of = (jnp.arange(count, dtype=jnp.int32) // per_dev).astype(jnp.int32)
        glob = ((owner[batch] * N_COL + column_of) * ROWS_DEV + obs_rows[batch]).astype(jnp.int32)
        obs_anom = anom[glob]
        obs_mean = mean[glob, 0]
        cov = jnp.dot(obs_anom, obs_anom.T, precision=lax.Precision.HIGHEST) / (members - 1.0)
        cov = cov + jnp.diag(obs_var[batch])
        cov_inv = invert_spd(cov)
        innov = obs_value[batch] - obs_mean
        blocks = jnp.repeat(jnp.repeat(taper_mask[batch], BLK, axis=0), BLK, axis=1)
        dist = jnp.abs(positions[:, None] - glob[None, :]).astype(jnp.float32)
        taper = blocks.astype(jnp.float32) * jnp.exp(-dist / jnp.float32(local_len))
        cross = jnp.dot(anom, obs_anom.T, precision=lax.Precision.HIGHEST) / (members - 1.0)
        gain = jnp.dot(taper * cross, cov_inv, precision=lax.Precision.HIGHEST)
        shift = jnp.dot(gain, innov[:, None], precision=lax.Precision.HIGHEST)
        change = jnp.dot(gain, obs_anom, precision=lax.Precision.HIGHEST)
        state = mean + shift + anom - 0.5 * change
    return state
```

```python
import functools

import jax
import jax.numpy as jnp
from jax import lax
from jax.experimental import pallas as pl
from jax.experimental.pallas import tpu as pltpu
from jax.sharding import PartitionSpec as P

HIGHEST = lax.Precision.HIGHEST
VMEM = pltpu.VMEM
SMEM = pltpu.SMEM
PIVOTS = 32


def spread(x, row):
    return jnp.broadcast_to(x[row : row + 1, :], (8, 128))


def sweep_panel(panel, base, lanes, subs):
    high = base >= 128
    q0 = base - jnp.where(high, 128, 0)
    low_half = [panel[8 * g : 8 * g + 8, :128] for g in range(4)]
    high_half = [panel[8 * g : 8 * g + 8, 128:] for g in range(4)]
    act = [jnp.where(high, h, l) for l, h in zip(low_half, high_half)]
    oth = [jnp.where(high, l, h) for l, h in zip(low_half, high_half)]
    for sb in range(4):
        cols = []
        for l in range(8):
            index = jnp.full((8, 128), q0 + (8 * sb + l), jnp.int32)
            cols.append([jnp.take_along_axis(act[g], index, axis=1) for g in range(4)])
        for l in range(8):
            u = cols[l]
            at_row = subs == l
            at_lane = lanes == q0 + (8 * sb + l)
            inv = 1.0 / spread(u[sb], l)
            for m in range(l + 1, 8):
                t = spread(cols[m][sb], l) * inv
                new = [cols[m][g] - u[g] * t for g in range(4)]
                new[sb] = jnp.where(at_row, t, new[sb])
                cols[m] = new
            row_act = jnp.where(at_lane, -inv, spread(act[sb], l) * inv)
            row_oth = spread(oth[sb], l) * inv
            act = [jnp.where(at_lane, 0.0, act[g]) - u[g] * row_act for g in range(4)]
            oth = [oth[g] - u[g] * row_oth for g in range(4)]
            act[sb] = jnp.where(at_row, row_act, act[sb])
            oth[sb] = jnp.where(at_row, row_oth, oth[sb])
    act, oth = jnp.concatenate(act, 0), jnp.concatenate(oth, 0)
    return jnp.concatenate(
        [jnp.where(high, oth, act), jnp.where(high, act, oth)], axis=1
    )


def invert_in_place(a_ref):
    n = a_ref.shape[0]
    lanes = lax.broadcasted_iota(jnp.int32, (8, 128), 1)
    subs = lax.broadcasted_iota(jnp.int32, (8, 128), 0)
    columns = lax.broadcasted_iota(jnp.int32, (n, n), 1)

    def outer(k, carry):
        base = pl.multiple_of(k * PIVOTS, PIVOTS)
        panel = a_ref[pl.ds(base, PIVOTS), :]
        swept = sweep_panel(panel, base, lanes, subs)
        prod = lax.dot_general(
            panel.T, swept, (((1,), (0,)), ((), ())), precision=HIGHEST,
            preferred_element_type=jnp.float32,
        )
        inside = (columns >= base) & (columns < base + PIVOTS)
        a_ref[...] = jnp.where(inside, 0.0, a_ref[...]) - prod
        a_ref[pl.ds(base, PIVOTS), :] = swept
        return carry

    lax.fori_loop(0, n // PIVOTS, outer, 0)


def dot_nt(a, b):
    return lax.dot_general(
        a, b, (((1,), (1,)), ((), ())), precision=HIGHEST,
        preferred_element_type=jnp.float32,
    )


def dot_nn(a, b):
    return jnp.dot(a, b, precision=HIGHEST, preferred_element_type=jnp.float32)


def pick_kernel(rows_ref, col_ref, mask_ref, x_ref, out_ref, held):
    rows_dev, members = x_ref.shape
    count = rows_ref.shape[1]
    per_dev = held.shape[0] // 2
    start = col_ref[0] * per_dev
    for b in range(2):
        for i in range(per_dev):
            r = rows_ref[b, start + i]
            held[b * per_dev + i : b * per_dev + i + 1, :] = x_ref[pl.ds(r, 1), :]
    chunks = members // 128
    subs = lax.broadcasted_iota(jnp.int32, (8, 128), 0)
    kept = jnp.where(subs == 0, mask_ref[0, 0, 0], mask_ref[0, 0, 1]).astype(jnp.float32)
    for piece in range(out_ref.shape[0]):
        g, j = piece // chunks, piece % chunks
        out_ref[piece, :8, :] = held[8 * g : 8 * g + 8, 128 * j : 128 * j + 128]
        out_ref[piece, 8:, :] = kept


def assimilate_kernel(
    place_ref, owner_ref, mask_ref, x_ref, own_ref, other_ref, kept_ref,
    rows_ref, rows_col_ref, value_col_ref, var_ref,
    out_ref, q_ref, t_ref, c_ref, g_ref, mean_ref,
    *, ncols, local_len,
):
    rows_dev, members = x_ref.shape
    n = rows_ref.shape[1]
    per_dev = n // ncols
    chunks = members // 128
    core, first = place_ref[0], place_ref[1]
    scale = 1.0 / (members - 1.0)
    obs1, obs0 = rows_dev, rows_dev + n

    def unpack(c, carry):
        for b, top in ((0, obs0), (1, obs1)):
            for gg in range(per_dev // 8):
                for jj in range(chunks // 2):
                    slot = (b * (per_dev // 8) + gg) * (chunks // 2) + jj
                    at = pl.ds(pl.multiple_of(top + c * per_dev + gg * 8, 8), 8)
                    mine = pl.multiple_of((2 * jj + core) * 128, 128)
                    theirs = pl.multiple_of((2 * jj + 1 - core) * 128, 128)
                    q_ref[at, pl.ds(mine, 128)] = own_ref[slot, c]
                    q_ref[at, pl.ds(theirs, 128)] = other_ref[slot, c]
        return carry

    lax.fori_loop(0, ncols, unpack, 0)
    q_ref[:rows_dev, :] = x_ref[...]

    def centre(i, carry):
        at = pl.ds(pl.multiple_of(i * 64, 64), 64)
        x = q_ref[at, :]
        mean = jnp.sum(x, axis=1, keepdims=True) * (1.0 / members)
        mean_ref[at, :] = jnp.broadcast_to(mean, (64, 128))
        q_ref[at, :] = x - mean
        return carry

    lax.fori_loop(0, q_ref.shape[0] // 64, centre, 0)

    lane = lax.broadcasted_iota(jnp.int32, (1, n), 1)
    glob = [(owner_ref[b] * ncols + lane // per_dev) * rows_dev + rows_ref[b : b + 1, :] for b in range(2)]
    diag = lax.broadcasted_iota(jnp.int32, (n, n), 0) == lax.broadcasted_iota(jnp.int32, (n, n), 1)
    here = first + lax.broadcasted_iota(jnp.int32, (rows_dev, 1), 0)
    sub = lax.broadcasted_iota(jnp.int32, (n, 1), 0)
    there = (owner_ref[1] * ncols + sub // per_dev) * rows_dev + rows_col_ref[:, 1:2]

    def decay(positions, b):
        dist = jnp.abs(positions - glob[b]).astype(jnp.float32)
        return jnp.exp(-dist / jnp.float32(local_len))

    def local_mask(b):
        return jnp.where(lane < 128, mask_ref[b, 0, 0], mask_ref[b, 0, 1]).astype(jnp.float32)

    def cross0(i, carry):
        at = pl.ds(pl.multiple_of(i * 128, 128), 128)
        t_ref[at, :] = dot_nt(q_ref[at, :], q_ref[obs0:, :]) * scale
        return carry

    lax.fori_loop(0, q_ref.shape[0] // 128, cross0, 0)
    c_ref[...] = t_ref[obs0:, :] + jnp.where(diag, var_ref[0:1, :], 0.0)
    invert_in_place(c_ref)

    t_ref[:rows_dev, :] = t_ref[:rows_dev, :] * (decay(here, 0) * local_mask(0))
    for c in range(ncols):
        at = slice(obs1 + c * per_dev, obs1 + (c + 1) * per_dev)
        kept = jnp.concatenate(
            [jnp.broadcast_to(kept_ref[c, i : i + 1, :], (per_dev, 128)) for i in range(2)], axis=1
        )
        t_ref[at, :] = t_ref[at, :] * (decay(there[c * per_dev : (c + 1) * per_dev], 0) * kept)
    innov0 = value_col_ref[:, 0:1] - mean_ref[obs0:, :]

    def update(i, carry):
        at = pl.ds(pl.multiple_of(i * 128, 128), 128)
        gain = -dot_nn(t_ref[at, :], c_ref[...])
        mean_ref[at, :] = mean_ref[at, :] + dot_nn(gain, innov0)
        q_ref[at, :] = q_ref[at, :] - 0.5 * dot_nn(gain, q_ref[obs0:, :])
        return carry

    lax.fori_loop(0, obs0 // 128, update, 0)

    def cross1(i, carry):
        at = pl.ds(pl.multiple_of(i * 128, 128), 128)
        t_ref[at, :] = dot_nt(q_ref[at, :], q_ref[obs1:obs0, :]) * scale
        return carry

    lax.fori_loop(0, obs0 // 128, cross1, 0)
    c_ref[...] = t_ref[obs1:obs0, :] + jnp.where(diag, var_ref[1:2, :], 0.0)
    invert_in_place(c_ref)
    innov1 = value_col_ref[:, 1:2] - mean_ref[obs1:obs0, :]
    tapered = t_ref[:rows_dev, :] * (decay(here, 1) * local_mask(1))
    gain = -dot_nn(tapered, c_ref[...])
    mean = mean_ref[:rows_dev, :] + dot_nn(gain, innov1)
    change = dot_nn(gain, q_ref[obs1:obs0, :])
    out_ref[...] = mean[:, 0:1] + q_ref[:rows_dev, :] - 0.5 * change


def to_all(x, axis, copies, groups=None):
    wide = jnp.broadcast_to(x[None], (copies, *x.shape))
    return lax.all_to_all(wide, axis, split_axis=0, concat_axis=0, axis_index_groups=groups, tiled=True)


def pick_rows(ensemble, obs_rows, taper_mask, my_col, per_dev):
    members = ensemble.shape[1]
    pieces = 2 * per_dev // 8 * (members // 128)
    return pl.pallas_call(
        pick_kernel,
        out_shape=jax.ShapeDtypeStruct((pieces, 16, 128), jnp.float32),
        in_specs=[pl.BlockSpec(memory_space=SMEM)] * 3 + [pl.BlockSpec(memory_space=VMEM)],
        out_specs=pl.BlockSpec(memory_space=VMEM),
        scratch_shapes=[VMEM((2 * per_dev, members), jnp.float32)],
        name="pick_rows",
    )(obs_rows, my_col[None], taper_mask, ensemble)


def assimilate(place, owner, taper_mask, ensemble, own, other, kept, obs_rows, obs_value, obs_var, ncols, local_len):
    rows_dev, members = ensemble.shape
    n = obs_rows.shape[1]
    total = rows_dev + 2 * n
    return pl.pallas_call(
        functools.partial(assimilate_kernel, ncols=ncols, local_len=local_len),
        out_shape=jax.ShapeDtypeStruct(ensemble.shape, jnp.float32),
        in_specs=[pl.BlockSpec(memory_space=SMEM)] * 3 + [pl.BlockSpec(memory_space=VMEM)] * 8,
        out_specs=pl.BlockSpec(memory_space=VMEM),
        scratch_shapes=[
            VMEM((total, members), jnp.float32),
            VMEM((total, n), jnp.float32),
            VMEM((n, n), jnp.float32),
            VMEM((8, 128), jnp.float32),
            VMEM((total, 128), jnp.float32),
        ],
        compiler_params=pltpu.CompilerParams(vmem_limit_bytes=40 * 1024 * 1024),
        name="assimilate",
    )(place, owner, taper_mask, ensemble, own, other, kept, obs_rows, obs_rows.T, obs_value.T, obs_var)


def gather_observed(ensemble, obs_rows, owner, taper_mask, my_row, my_col, nrows, ncols):
    per_dev = obs_rows.shape[1] // ncols
    picked = pick_rows(ensemble, obs_rows, taper_mask, my_col, per_dev)
    spread_out = lax.all_to_all(picked, "row", split_axis=0, concat_axis=0, tiled=True)
    batch = my_row // (nrows // 2)
    data = lax.dynamic_index_in_dim(spread_out, owner[batch], 0, keepdims=False)[:8]
    kept = lax.dynamic_index_in_dim(spread_out, owner[1], 0, keepdims=False)[8:]
    line = to_all(jnp.concatenate([data, kept], 0), "col", ncols)
    line = line.reshape(ncols, 16, 128)
    same_core = [[r for r in range(nrows) if r % 2 == c] for c in range(2)]
    own = to_all(line[:, :8], "row", nrows // 2, same_core).reshape(nrows // 2, ncols, 8, 128)
    other = lax.ppermute(own, "row", [(r, r ^ 1) for r in range(nrows)])
    return own, other, line[:, 8:]


def on_device(ensemble, obs_rows, owner, obs_value, obs_var, taper_mask):
    rows = ensemble.shape[0]
    ncols, nrows = lax.axis_size("col"), lax.axis_size("row")
    my_row, my_col = lax.axis_index("row"), lax.axis_index("col")
    own, other, kept = gather_observed(ensemble, obs_rows, owner, taper_mask, my_row, my_col, nrows, ncols)
    local_len = rows * nrows * ncols // 4
    place = jnp.stack([my_row % 2, (my_row * ncols + my_col) * rows]).astype(jnp.int32)
    return assimilate(place, owner, taper_mask, ensemble, own, other, kept, obs_rows, obs_value, obs_var, ncols, local_len)


def solution(mesh):
    in_specs = (P(("row", "col"), None), P(), P(), P(), P(), P(None, ("row", "col"), None))
    out_specs = P(("row", "col"), None)
    return jax.shard_map(
        on_device, mesh=mesh, in_specs=in_specs, out_specs=out_specs, check_vma=False
    )
```

```python
import functools

import jax
import jax.numpy as jnp
from jax import lax
from jax.experimental import pallas as pl
from jax.experimental.pallas import tpu as pltpu
from jax.sharding import PartitionSpec as P

VMEM = pltpu.VMEM
SMEM = pltpu.SMEM
PIVOTS = 32
TERMS = ((0, 0), (0, 1), (1, 0), (1, 1), (0, 2), (2, 0))


def split(x, parts):
    out = []
    for i in range(parts):
        out.append(x.astype(jnp.bfloat16))
        if i < parts - 1:
            x = x - out[-1].astype(jnp.float32)
    return out


def dot_parts(a, b, contract):
    pairs = TERMS[: 3 if len(a) == 2 else 6]
    left = jnp.concatenate([a[i] for i, _ in pairs], axis=1)
    right = jnp.concatenate([b[j] for _, j in pairs], axis=contract)
    return lax.dot_general(
        left, right, (((1,), (contract,)), ((), ())), preferred_element_type=jnp.float32
    )


def by_terms(x, side):
    parts = split(x, 3)
    return jnp.concatenate([parts[term[side]] for term in TERMS], axis=0)


def one_pass(a, b):
    return jnp.dot(a, b, preferred_element_type=jnp.float32)


def spread(x, row):
    return jnp.broadcast_to(x[row : row + 1, :], (8, 128))


def sweep_panel(panel, base, lanes, subs):
    high = base >= 128
    q0 = base - jnp.where(high, 128, 0)
    low_half = [panel[8 * g : 8 * g + 8, :128] for g in range(4)]
    high_half = [panel[8 * g : 8 * g + 8, 128:] for g in range(4)]
    act = [jnp.where(high, h, l) for l, h in zip(low_half, high_half)]
    oth = [jnp.where(high, l, h) for l, h in zip(low_half, high_half)]

    def column(g, c):
        return jnp.take_along_axis(act[g], jnp.full((8, 128), q0 + c, jnp.int32), axis=1)

    diag = [column(0, l) for l in range(8)]
    for sb in range(4):
        cols = [[None] * 4 for _ in range(8)]
        later = [g for g in range(sb + 1, 4)] + [g for g in range(sb)]
        for g in later[:1]:
            for l in range(8):
                cols[l][g] = column(g, 8 * sb + l)
        following = [column(sb + 1, 8 * sb + 8 + l) for l in range(8)] if sb < 3 else None
        for g in later[1:]:
            for l in range(8):
                cols[l][g] = column(g, 8 * sb + l)
        invs, factors = [], [[None] * 8 for _ in range(8)]
        for l in range(8):
            at_row = subs == l
            inv = 1.0 / spread(diag[l], l)
            invs.append(inv)
            for m in range(l + 1, 8):
                t = spread(diag[m], l) * inv
                factors[l][m] = t
                diag[m] = jnp.where(at_row, t, diag[m] - diag[l] * t)
        for l in range(8):
            cols[l][sb] = diag[l]
        for g in later:
            for l in range(8):
                for m in range(l + 1, 8):
                    cols[m][g] = cols[m][g] - cols[l][g] * factors[l][m]
        if sb < 3:
            for l in range(8):
                scaled = cols[l][sb + 1] * invs[l]
                following = [f - cols[l][sb + 1] * spread(scaled, m) for m, f in enumerate(following)]
        for l in range(8):
            u = cols[l]
            at_row = subs == l
            at_lane = lanes == q0 + (8 * sb + l)
            inv = invs[l]
            row_act = jnp.where(at_lane, -inv, spread(act[sb], l) * inv)
            row_oth = spread(oth[sb], l) * inv
            act = [jnp.where(at_lane, 0.0, act[g]) - u[g] * row_act for g in range(4)]
            oth = [oth[g] - u[g] * row_oth for g in range(4)]
            act[sb] = jnp.where(at_row, row_act, act[sb])
            oth[sb] = jnp.where(at_row, row_oth, oth[sb])
        diag = following
    act, oth = jnp.concatenate(act, 0), jnp.concatenate(oth, 0)
    return jnp.concatenate(
        [jnp.where(high, oth, act), jnp.where(high, act, oth)], axis=1
    )


def invert_in_place(a_ref, panel_ref, swept_ref, trans_ref, beside):
    n = a_ref.shape[0]
    steps = n // PIVOTS
    lanes = lax.broadcasted_iota(jnp.int32, (8, 128), 1)
    subs = lax.broadcasted_iota(jnp.int32, (8, 128), 0)
    columns = lax.broadcasted_iota(jnp.int32, (n, n), 1)

    def inside(k, rows):
        return (columns[:rows] >= k * PIVOTS) & (columns[:rows] < (k + 1) * PIVOTS)

    def rows_of(k):
        return pl.ds(pl.multiple_of(k * PIVOTS, PIVOTS), PIVOTS)

    def apply(k, slot):
        a_ref[...] = jnp.where(inside(k, n), 0.0, a_ref[...]) - one_pass(
            trans_ref[slot], by_terms(swept_ref[slot], 1)
        )

    panel_ref[...] = a_ref[:PIVOTS, :]
    swept_ref[1] = jnp.zeros_like(panel_ref)
    trans_ref[1] = jnp.zeros(trans_ref.shape[1:], jnp.bfloat16)

    def step(k, carry):
        now, before = k % 2, (k + 1) % 2
        panel = panel_ref[...]
        trans_ref[now] = by_terms(panel, 0).T
        swept = sweep_panel(panel, k * PIVOTS, lanes, subs)
        apply(k - 1, before)
        last = jnp.maximum(k - 1, 0)
        a_ref[rows_of(last), :] = jnp.where(k > 0, swept_ref[before], a_ref[rows_of(last), :])
        beside(k)
        following = jnp.minimum(k + 1, steps - 1)
        panel_ref[...] = jnp.where(inside(k, PIVOTS), 0.0, a_ref[rows_of(following), :]) - one_pass(
            trans_ref[now, rows_of(following), :], by_terms(swept, 1)
        )
        swept_ref[now] = swept
        return carry

    lax.fori_loop(0, steps, step, 0)
    final = (steps - 1) % 2
    apply(steps - 1, final)
    a_ref[n - PIVOTS :, :] = swept_ref[final]


def pick_kernel(rows_ref, col_ref, mask_ref, x_ref, out_ref, held):
    rows_dev, members = x_ref.shape
    count = rows_ref.shape[1]
    per_dev = held.shape[0] // 2
    start = col_ref[0] * per_dev
    for b in range(2):
        for i in range(per_dev):
            r = rows_ref[b, start + i]
            held[b * per_dev + i : b * per_dev + i + 1, :] = x_ref[pl.ds(r, 1), :]
    chunks = members // 128
    subs = lax.broadcasted_iota(jnp.int32, (8, 128), 0)
    kept = jnp.where(subs == 0, mask_ref[0, 0, 0], mask_ref[0, 0, 1]).astype(jnp.float32)
    for piece in range(out_ref.shape[0]):
        g, j = piece // chunks, piece % chunks
        out_ref[piece, :8, :] = held[8 * g : 8 * g + 8, 128 * j : 128 * j + 128]
        out_ref[piece, 8:, :] = kept


def assimilate_kernel(
    place_ref, owner_ref, mask_ref, x_ref, own_ref, other_ref, kept_ref,
    rows_ref, rows_col_ref, value_col_ref, var_ref,
    out_ref, q_ref, s0_ref, s1_ref, t_ref, c_ref, g_ref, mean_ref, panel_ref, swept_ref, trans_ref,
    v_ref, innov_ref,
    *, ncols, local_len,
):
    rows_dev, members = x_ref.shape
    n = rows_ref.shape[1]
    per_dev = n // ncols
    chunks = members // 128
    core, first = place_ref[0], place_ref[1]
    scale = 1.0 / (members - 1.0)
    obs1, obs0 = rows_dev, rows_dev + n

    def unpack(c, carry):
        for b, top in ((0, obs0), (1, obs1)):
            for gg in range(per_dev // 8):
                at = pl.ds(pl.multiple_of(top + c * per_dev + gg * 8, 8), 8)
                total = jnp.zeros((8, 128), jnp.float32)
                for jj in range(chunks // 2):
                    slot = (b * (per_dev // 8) + gg) * (chunks // 2) + jj
                    mine = pl.multiple_of((2 * jj + core) * 128, 128)
                    theirs = pl.multiple_of((2 * jj + 1 - core) * 128, 128)
                    q_ref[at, pl.ds(mine, 128)] = own_ref[slot, c]
                    q_ref[at, pl.ds(theirs, 128)] = other_ref[slot, c]
                    total = total + (own_ref[slot, c] + other_ref[slot, c])
                mean_ref[at, :] = total
        return carry

    lax.fori_loop(0, ncols, unpack, 0)
    total = x_ref[:, :128]
    for j in range(1, chunks):
        total = total + x_ref[:, 128 * j : 128 * j + 128]
    mean_ref[:rows_dev, :] = total
    mean = jnp.sum(mean_ref[...], axis=1, keepdims=True) * (1.0 / members)
    mean_ref[...] = jnp.broadcast_to(mean, mean_ref.shape)

    def chunk(j, width):
        return pl.ds(pl.multiple_of(j * width, width), width)

    wide = 2 * 128
    diag = lax.broadcasted_iota(jnp.int32, (n, n), 0) == lax.broadcasted_iota(jnp.int32, (n, n), 1)
    c_ref[...] = jnp.where(diag, var_ref[0:1, :], 0.0)

    def covariance0(j, carry):
        at = chunk(j, wide)
        anom = q_ref[obs0:, at] - jnp.concatenate([mean_ref[obs0:, :]] * 2, axis=1)
        parts = split(anom, 3)
        for i in range(3):
            s0_ref[i, :, at] = parts[i]
        c_ref[...] += dot_parts(parts, parts, 1) * scale
        return carry

    lax.fori_loop(0, members // wide, covariance0, 0)
    t_ref[...] = jnp.zeros_like(t_ref)

    def cross0(j):
        at = chunk(j, 128)
        for top, rows, src in ((0, rows_dev, x_ref), (obs1, n, q_ref)):
            anom = src[top : top + rows, at] - mean_ref[top : top + rows, :]
            q_ref[top : top + rows, at] = anom
            t_ref[top : top + rows, :] += dot_parts(
                split(anom, 3), [s0_ref[i, :, at] for i in range(3)], 1
            )

    invert_in_place(c_ref, panel_ref, swept_ref, trans_ref, cross0)

    lane = lax.broadcasted_iota(jnp.int32, (1, n), 1)
    glob = [(owner_ref[b] * ncols + lane // per_dev) * rows_dev + rows_ref[b : b + 1, :] for b in range(2)]
    here = first + lax.broadcasted_iota(jnp.int32, (rows_dev, 1), 0)
    sub = lax.broadcasted_iota(jnp.int32, (n, 1), 0)
    there = (owner_ref[1] * ncols + sub // per_dev) * rows_dev + rows_col_ref[:, 1:2]

    def decay(positions, b):
        dist = jnp.abs(positions - glob[b]).astype(jnp.float32)
        return jnp.exp(-dist / jnp.float32(local_len)) * -scale

    def local_mask(b):
        return jnp.where(lane < 128, mask_ref[b, 0, 0], mask_ref[b, 0, 1]).astype(jnp.float32)

    t_ref[:rows_dev, :] = t_ref[:rows_dev, :] * (decay(here, 0) * local_mask(0))
    for c in range(ncols):
        at = slice(obs1 + c * per_dev, obs1 + (c + 1) * per_dev)
        kept = jnp.concatenate(
            [jnp.broadcast_to(kept_ref[c, i : i + 1, :], (per_dev, 128)) for i in range(2)], axis=1
        )
        t_ref[at, :] = t_ref[at, :] * (decay(there[c * per_dev : (c + 1) * per_dev], 0) * kept)
    for p, part in enumerate(split(c_ref[...], 3)):
        v_ref[p] = part

    def gain(at, parts):
        return split(dot_parts(split(t_ref[at, :], 3), [v_ref[i] for i in range(3)], 0), parts)

    def gain0(i, carry):
        at = chunk(i, 128)
        for p, part in enumerate(gain(at, 3)):
            g_ref[p, at, :] = part
        return carry

    lax.fori_loop(0, obs0 // 128, gain0, 0)
    for p, part in enumerate(split(value_col_ref[:, 0:1] - mean_ref[obs0:, :], 3)):
        innov_ref[p] = part

    c_ref[...] = jnp.where(diag, var_ref[1:2, :], 0.0)

    def covariance1(j, carry):
        at = chunk(j, wide)
        change = dot_parts(
            [g_ref[i, obs1:obs0, :] for i in range(3)], [s0_ref[i, :, at] for i in range(3)], 0
        )
        parts = split(q_ref[obs1:obs0, at] - 0.5 * change, 3)
        for i in range(3):
            s1_ref[i, :, at] = parts[i]
        c_ref[...] += dot_parts(parts, parts, 1) * scale
        return carry

    lax.fori_loop(0, members // wide, covariance1, 0)
    t_ref[:rows_dev, :] = jnp.zeros((rows_dev, n), jnp.float32)

    def cross1(j):
        at = chunk(j, 128)
        some = chunk(j, obs0 // (members // 128))
        mean_ref[some, :] += dot_parts(
            [g_ref[i, some, :] for i in range(3)], [innov_ref[i] for i in range(3)], 0
        )
        change = dot_parts(
            [g_ref[i, :rows_dev, :] for i in range(2)], [s0_ref[i, :, at] for i in range(2)], 0
        )
        anom = q_ref[:rows_dev, at] - 0.5 * change
        q_ref[:rows_dev, at] = anom
        t_ref[:rows_dev, :] += dot_parts(
            split(anom, 3), [s1_ref[i, :, at] for i in range(3)], 1
        )

    invert_in_place(c_ref, panel_ref, swept_ref, trans_ref, cross1)
    innov1 = split(value_col_ref[:, 1:2] - mean_ref[obs1:obs0, :], 2)
    t_ref[:rows_dev, :] = t_ref[:rows_dev, :] * (decay(here, 1) * local_mask(1))
    for p, part in enumerate(split(c_ref[...], 3)):
        v_ref[p] = part
    gain1 = gain(slice(0, rows_dev), 2)
    mean = mean_ref[:rows_dev, :] + dot_parts(gain1, innov1, 0)
    for j in range(members // wide):
        at = slice(j * wide, (j + 1) * wide)
        change = dot_parts(gain1, [s1_ref[i, :, at] for i in range(2)], 0)
        out_ref[:, at] = jnp.concatenate([mean] * 2, axis=1) + q_ref[:rows_dev, at] - 0.5 * change


def to_all(x, axis, copies, groups=None):
    wide = jnp.broadcast_to(x[None], (copies, *x.shape))
    return lax.all_to_all(wide, axis, split_axis=0, concat_axis=0, axis_index_groups=groups, tiled=True)


def pick_rows(ensemble, obs_rows, taper_mask, my_col, per_dev):
    members = ensemble.shape[1]
    pieces = 2 * per_dev // 8 * (members // 128)
    return pl.pallas_call(
        pick_kernel,
        out_shape=jax.ShapeDtypeStruct((pieces, 16, 128), jnp.float32),
        in_specs=[pl.BlockSpec(memory_space=SMEM)] * 3 + [pl.BlockSpec(memory_space=VMEM)],
        out_specs=pl.BlockSpec(memory_space=VMEM),
        scratch_shapes=[VMEM((2 * per_dev, members), jnp.float32)],
        name="pick_rows",
    )(obs_rows, my_col[None], taper_mask, ensemble)


def assimilate(place, owner, taper_mask, ensemble, own, other, kept, obs_rows, obs_value, obs_var, ncols, local_len):
    rows_dev, members = ensemble.shape
    n = obs_rows.shape[1]
    total = rows_dev + 2 * n
    return pl.pallas_call(
        functools.partial(assimilate_kernel, ncols=ncols, local_len=local_len),
        out_shape=jax.ShapeDtypeStruct(ensemble.shape, jnp.float32),
        in_specs=[pl.BlockSpec(memory_space=SMEM)] * 3 + [pl.BlockSpec(memory_space=VMEM)] * 8,
        out_specs=pl.BlockSpec(memory_space=VMEM),
        scratch_shapes=[
            VMEM((total, members), jnp.float32),
            VMEM((3, n, members), jnp.bfloat16),
            VMEM((3, n, members), jnp.bfloat16),
            VMEM((rows_dev + n, n), jnp.float32),
            VMEM((n, n), jnp.float32),
            VMEM((3, rows_dev + n, n), jnp.bfloat16),
            VMEM((total, 128), jnp.float32),
            VMEM((PIVOTS, n), jnp.float32),
            VMEM((2, PIVOTS, n), jnp.float32),
            VMEM((2, n, len(TERMS) * PIVOTS), jnp.bfloat16),
            VMEM((3, n, n), jnp.bfloat16),
            VMEM((3, n, 128), jnp.bfloat16),
        ],
        compiler_params=pltpu.CompilerParams(vmem_limit_bytes=40 * 1024 * 1024),
        name="assimilate",
    )(place, owner, taper_mask, ensemble, own, other, kept, obs_rows, obs_rows.T, obs_value.T, obs_var)


def gather_observed(ensemble, obs_rows, owner, taper_mask, my_row, my_col, nrows, ncols):
    per_dev = obs_rows.shape[1] // ncols
    picked = pick_rows(ensemble, obs_rows, taper_mask, my_col, per_dev)
    spread_out = lax.all_to_all(picked, "row", split_axis=0, concat_axis=0, tiled=True)
    batch = my_row // (nrows // 2)
    data = lax.dynamic_index_in_dim(spread_out, owner[batch], 0, keepdims=False)[:8]
    kept = lax.dynamic_index_in_dim(spread_out, owner[1], 0, keepdims=False)[8:]
    line = to_all(jnp.concatenate([data, kept], 0), "col", ncols)
    line = line.reshape(ncols, 16, 128)
    same_core = [[r for r in range(nrows) if r % 2 == c] for c in range(2)]
    own = to_all(line[:, :8], "row", nrows // 2, same_core).reshape(nrows // 2, ncols, 8, 128)
    other = lax.ppermute(own, "row", [(r, r ^ 1) for r in range(nrows)])
    return own, other, line[:, 8:]


def on_device(ensemble, obs_rows, owner, obs_value, obs_var, taper_mask):
    rows = ensemble.shape[0]
    ncols, nrows = lax.axis_size("col"), lax.axis_size("row")
    my_row, my_col = lax.axis_index("row"), lax.axis_index("col")
    own, other, kept = gather_observed(ensemble, obs_rows, owner, taper_mask, my_row, my_col, nrows, ncols)
    local_len = rows * nrows * ncols // 4
    place = jnp.stack([my_row % 2, (my_row * ncols + my_col) * rows]).astype(jnp.int32)
    return assimilate(place, owner, taper_mask, ensemble, own, other, kept, obs_rows, obs_value, obs_var, ncols, local_len)


def solution(mesh):
    in_specs = (P(("row", "col"), None), P(), P(), P(), P(), P(None, ("row", "col"), None))
    out_specs = P(("row", "col"), None)
    return jax.shard_map(
        on_device, mesh=mesh, in_specs=in_specs, out_specs=out_specs, check_vma=False
    )
```

```python
import functools

import jax
import jax.numpy as jnp
from jax import lax
from jax.experimental import pallas as pl
from jax.experimental.pallas import tpu as pltpu
from jax.sharding import PartitionSpec as P

VMEM = pltpu.VMEM
SMEM = pltpu.SMEM
PIVOTS = 32
TERMS = ((0, 0), (0, 1), (1, 0), (1, 1), (0, 2), (2, 0))


def split(x, parts):
    out = []
    for i in range(parts):
        out.append(x.astype(jnp.bfloat16))
        if i < parts - 1:
            x = x - out[-1].astype(jnp.float32)
    return out


def dot_parts(a, b, contract):
    pairs = TERMS[: 3 if len(a) == 2 else 6]
    left = jnp.concatenate([a[i] for i, _ in pairs], axis=1)
    right = jnp.concatenate([b[j] for _, j in pairs], axis=contract)
    return lax.dot_general(
        left, right, (((1,), (contract,)), ((), ())), preferred_element_type=jnp.float32
    )


def by_terms(x, side):
    parts = split(x, 3)
    return jnp.concatenate([parts[term[side]] for term in TERMS], axis=0)


def one_pass(a, b):
    return jnp.dot(a, b, preferred_element_type=jnp.float32)


def spread(x, row):
    return jnp.broadcast_to(x[row : row + 1, :], (8, 128))


def sweep_panel(panel, base, lanes, subs):
    high = base >= 128
    q0 = base - jnp.where(high, 128, 0)
    low_half = [panel[8 * g : 8 * g + 8, :128] for g in range(4)]
    high_half = [panel[8 * g : 8 * g + 8, 128:] for g in range(4)]
    act = [jnp.where(high, h, l) for l, h in zip(low_half, high_half)]
    oth = [jnp.where(high, l, h) for l, h in zip(low_half, high_half)]

    def column(g, c):
        return jnp.take_along_axis(act[g], jnp.full((8, 128), q0 + c, jnp.int32), axis=1)

    diag = [column(0, l) for l in range(8)]
    for sb in range(4):
        cols = [[None] * 4 for _ in range(8)]
        later = [g for g in range(sb + 1, 4)] + [g for g in range(sb)]
        for g in later[:1]:
            for l in range(8):
                cols[l][g] = column(g, 8 * sb + l)
        following = [column(sb + 1, 8 * sb + 8 + l) for l in range(8)] if sb < 3 else None
        for g in later[1:]:
            for l in range(8):
                cols[l][g] = column(g, 8 * sb + l)
        invs, factors = [], [[None] * 8 for _ in range(8)]
        for l in range(8):
            at_row = subs == l
            inv = 1.0 / spread(diag[l], l)
            invs.append(inv)
            for m in range(l + 1, 8):
                t = spread(diag[m], l) * inv
                factors[l][m] = t
                diag[m] = jnp.where(at_row, t, diag[m] - diag[l] * t)
        for l in range(8):
            cols[l][sb] = diag[l]
        for g in later:
            for l in range(8):
                for m in range(l + 1, 8):
                    cols[m][g] = cols[m][g] - cols[l][g] * factors[l][m]
        if sb < 3:
            for l in range(8):
                scaled = cols[l][sb + 1] * invs[l]
                following = [f - cols[l][sb + 1] * spread(scaled, m) for m, f in enumerate(following)]
        for l in range(8):
            u = cols[l]
            at_row = subs == l
            at_lane = lanes == q0 + (8 * sb + l)
            inv = invs[l]
            row_act = jnp.where(at_lane, -inv, spread(act[sb], l) * inv)
            row_oth = spread(oth[sb], l) * inv
            act = [jnp.where(at_lane, 0.0, act[g]) - u[g] * row_act for g in range(4)]
            oth = [oth[g] - u[g] * row_oth for g in range(4)]
            act[sb] = jnp.where(at_row, row_act, act[sb])
            oth[sb] = jnp.where(at_row, row_oth, oth[sb])
        diag = following
    act, oth = jnp.concatenate(act, 0), jnp.concatenate(oth, 0)
    return jnp.concatenate(
        [jnp.where(high, oth, act), jnp.where(high, act, oth)], axis=1
    )


def invert_in_place(a_ref, panel_ref, swept_ref, trans_ref, beside):
    n = a_ref.shape[0]
    steps = n // PIVOTS
    lanes = lax.broadcasted_iota(jnp.int32, (8, 128), 1)
    subs = lax.broadcasted_iota(jnp.int32, (8, 128), 0)
    columns = lax.broadcasted_iota(jnp.int32, (n, n), 1)

    def inside(k, rows):
        return (columns[:rows] >= k * PIVOTS) & (columns[:rows] < (k + 1) * PIVOTS)

    def rows_of(k):
        return pl.ds(pl.multiple_of(k * PIVOTS, PIVOTS), PIVOTS)

    def apply(k, slot):
        a_ref[...] = jnp.where(inside(k, n), 0.0, a_ref[...]) - one_pass(
            trans_ref[slot], by_terms(swept_ref[slot], 1)
        )

    panel_ref[...] = a_ref[:PIVOTS, :]
    swept_ref[1] = jnp.zeros_like(panel_ref)
    trans_ref[1] = jnp.zeros(trans_ref.shape[1:], jnp.bfloat16)

    def step(k, carry):
        now, before = k % 2, (k + 1) % 2
        panel = panel_ref[...]
        trans_ref[now] = by_terms(panel, 0).T
        swept = sweep_panel(panel, k * PIVOTS, lanes, subs)
        apply(k - 1, before)
        last = jnp.maximum(k - 1, 0)
        a_ref[rows_of(last), :] = jnp.where(k > 0, swept_ref[before], a_ref[rows_of(last), :])
        beside(k)
        following = jnp.minimum(k + 1, steps - 1)
        panel_ref[...] = jnp.where(inside(k, PIVOTS), 0.0, a_ref[rows_of(following), :]) - one_pass(
            trans_ref[now, rows_of(following), :], by_terms(swept, 1)
        )
        swept_ref[now] = swept
        return carry

    lax.fori_loop(0, steps, step, 0)
    final = (steps - 1) % 2
    apply(steps - 1, final)
    a_ref[n - PIVOTS :, :] = swept_ref[final]


def pick_kernel(rows_ref, col_ref, mask_ref, x_ref, out_ref, held):
    members = x_ref.shape[1]
    per_dev = held.shape[0] // 2
    start = col_ref[0] * per_dev
    for b in range(2):
        for i in range(per_dev):
            r = rows_ref[b, start + i]
            held[b * per_dev + i : b * per_dev + i + 1, :] = x_ref[pl.ds(r, 1), :]
    chunks = members // 128
    lanes = lax.broadcasted_iota(jnp.int32, (1, 128), 1)
    kept = jnp.where(lanes == 0, mask_ref[0, 0, 0], mask_ref[0, 0, 1]).astype(jnp.float32)
    for piece in range(out_ref.shape[0]):
        g, j = piece // chunks, piece % chunks
        for s in range(8):
            out_ref[piece, :, 128 * s : 128 * s + 128] = held[8 * g + s : 8 * g + s + 1, 128 * j : 128 * j + 128]
        out_ref[piece, :, 1024:] = kept


def forward_kernel(source_ref, pieces_ref, out_ref):
    for s in range(9):
        at = slice(128 * s, 128 * s + 128)
        line = pieces_ref[source_ref[0 if s < 8 else 1], :, at]
        for d in range(out_ref.shape[0]):
            out_ref[d, :, at] = line


def share_kernel(line_ref, out_ref, kept_ref, held):
    for c in range(line_ref.shape[0]):
        for s in range(8):
            held[c, s : s + 1, :] = line_ref[c, :, 128 * s : 128 * s + 128]
        kept_ref[c : c + 1, :] = line_ref[c, :, 1024:]
    for d in range(out_ref.shape[0]):
        out_ref[d] = held[...]


def prepare_kernel(
    place_ref, owner_ref, mask_ref, x_ref, rows_ref, rows_col_ref, value_col_ref, var_ref,
    rho_ref, decay_ref, anom_ref, mean_ref, value_ref, held_var_ref, *, ncols, local_len,
):
    rows_dev, members = x_ref.shape
    n = rows_ref.shape[1]
    per_dev = n // ncols
    lane = lax.broadcasted_iota(jnp.int32, (1, n), 1)
    here = place_ref[1] + lax.broadcasted_iota(jnp.int32, (rows_dev, 1), 0)
    sub = lax.broadcasted_iota(jnp.int32, (n, 1), 0)
    there = (owner_ref[1] * ncols + sub // per_dev) * rows_dev + rows_col_ref[:, 1:2]

    def decay(positions, b):
        glob = (owner_ref[b] * ncols + lane // per_dev) * rows_dev + rows_ref[b : b + 1, :]
        dist = jnp.abs(positions - glob).astype(jnp.float32)
        return jnp.exp(-dist / jnp.float32(local_len))

    for b in range(2):
        mask = jnp.where(lane < 128, mask_ref[b, 0, 0], mask_ref[b, 0, 1]).astype(jnp.float32)
        rho_ref[b] = decay(here, b) * mask
    decay_ref[...] = decay(there, 0)
    x = x_ref[...]
    mean = jnp.sum(x, axis=1, keepdims=True) * (1.0 / members)
    anom_ref[...] = x - mean
    mean_ref[...] = jnp.broadcast_to(mean, mean_ref.shape)
    held = lax.broadcasted_iota(jnp.int32, value_ref.shape, 1)
    value_ref[...] = jnp.where(held == 0, value_col_ref[:, 0:1], value_col_ref[:, 1:2])
    held_var_ref[...] = var_ref[...]


def assimilate_kernel(
    place_ref, own_ref, other_ref, kept_ref, rho_ref, decay_ref, x_ref, x_mean_ref, value_ref, var_ref,
    out_ref, q_ref, s0_ref, s1_ref, t_ref, c_ref, g_ref, mean_ref, panel_ref, swept_ref, trans_ref,
    v_ref, innov_ref, stage_ref, sems,
):
    rows_dev, members = x_ref.shape
    n = var_ref.shape[1]
    ncols = kept_ref.shape[0]
    per_dev = n // ncols
    groups = per_dev // 8
    chunks = members // 128
    core = place_ref[0]
    scale = 1.0 / (members - 1.0)
    obs1, obs0 = rows_dev, rows_dev + n

    def member_chunk(i, side):
        return pl.ds(pl.multiple_of((2 * i + (core if side == 0 else 1 - core)) * 128, 128), 128)

    def chunk(j, width):
        return pl.ds(pl.multiple_of(j * width, width), width)

    def observed(b, i, ref):
        return jnp.concatenate(
            [ref[(b * groups + g) * (chunks // 2) + i, c] for c in range(ncols) for g in range(groups)], axis=0
        )

    def add_up(c, carry):
        for b, top in ((0, obs0), (1, obs1)):
            for g in range(groups):
                slots = [(b * groups + g) * (chunks // 2) + i for i in range(chunks // 2)]
                total = own_ref[slots[0], c] + other_ref[slots[0], c]
                for slot in slots[1:]:
                    total = total + (own_ref[slot, c] + other_ref[slot, c])
                mean_ref[pl.ds(pl.multiple_of(top + c * per_dev + g * 8, 8), 8), :] = total
        return carry

    lax.fori_loop(0, ncols, add_up, 0)
    mean = jnp.sum(mean_ref[obs1:, :], axis=1, keepdims=True) * (1.0 / members)
    mean_ref[obs1:, :] = jnp.broadcast_to(mean, (2 * n, 128))
    mean_ref[:rows_dev, :] = x_mean_ref[...]

    wide = 2 * 128
    diag = lax.broadcasted_iota(jnp.int32, (n, n), 0) == lax.broadcasted_iota(jnp.int32, (n, n), 1)
    c_ref[...] = jnp.where(diag, var_ref[0:1, :], 0.0)

    def covariance0(i, carry):
        mean = mean_ref[obs0:, :]
        anom = jnp.concatenate([observed(0, i, own_ref) - mean, observed(0, i, other_ref) - mean], axis=1)
        parts = split(anom, 3)
        for p in range(3):
            s0_ref[p, :, chunk(i, wide)] = parts[p]
        c_ref[...] += dot_parts(parts, parts, 1) * scale
        return carry

    lax.fori_loop(0, members // wide, covariance0, 0)
    t_ref[...] = jnp.zeros_like(t_ref)

    def cross0(j):
        at, i, side = chunk(j, 128), j // 2, j % 2
        local = jnp.where(side == 0, x_ref[:, member_chunk(i, 0)], x_ref[:, member_chunk(i, 1)])
        seen = jnp.where(side == 0, observed(1, i, own_ref), observed(1, i, other_ref))
        for top, anom in ((0, local), (obs1, seen - mean_ref[obs1:obs0, :])):
            rows = slice(top, top + anom.shape[0])
            q_ref[rows, at] = anom
            t_ref[rows, :] += dot_parts(split(anom, 3), [s0_ref[p, :, at] for p in range(3)], 1)

    invert_in_place(c_ref, panel_ref, swept_ref, trans_ref, cross0)

    t_ref[:rows_dev, :] = t_ref[:rows_dev, :] * (rho_ref[0] * -scale)
    for c in range(ncols):
        at = slice(obs1 + c * per_dev, obs1 + (c + 1) * per_dev)
        kept = jnp.concatenate(
            [jnp.broadcast_to(kept_ref[c : c + 1, i : i + 1] * -scale, (per_dev, 128)) for i in range(2)], axis=1
        )
        t_ref[at, :] = t_ref[at, :] * (decay_ref[c * per_dev : (c + 1) * per_dev, :] * kept)
    for p, part in enumerate(split(c_ref[...], 3)):
        v_ref[p] = part

    def gain(at, parts):
        return split(dot_parts(split(t_ref[at, :], 3), [v_ref[p] for p in range(3)], 0), parts)

    def gain0(i, carry):
        at = chunk(i, 128)
        for p, part in enumerate(gain(at, 3)):
            g_ref[p, at, :] = part
        return carry

    lax.fori_loop(0, obs0 // 128, gain0, 0)
    for p, part in enumerate(split(value_ref[:, 0:1] - mean_ref[obs0:, :], 3)):
        innov_ref[p] = part

    c_ref[...] = jnp.where(diag, var_ref[1:2, :], 0.0)

    def covariance1(i, carry):
        at = chunk(i, wide)
        change = dot_parts(
            [g_ref[p, obs1:obs0, :] for p in range(3)], [s0_ref[p, :, at] for p in range(3)], 0
        )
        parts = split(q_ref[obs1:obs0, at] - 0.5 * change, 3)
        for p in range(3):
            s1_ref[p, :, at] = parts[p]
        c_ref[...] += dot_parts(parts, parts, 1) * scale
        return carry

    lax.fori_loop(0, members // wide, covariance1, 0)
    t_ref[:rows_dev, :] = jnp.zeros((rows_dev, n), jnp.float32)

    def cross1(j):
        at = chunk(j, 128)
        some = chunk(j, obs0 // chunks)
        mean_ref[some, :] += dot_parts(
            [g_ref[p, some, :] for p in range(3)], [innov_ref[p] for p in range(3)], 0
        )
        change = dot_parts(
            [g_ref[p, :rows_dev, :] for p in range(2)], [s0_ref[p, :, at] for p in range(2)], 0
        )
        anom = q_ref[:rows_dev, at] - 0.5 * change
        q_ref[:rows_dev, at] = anom
        t_ref[:rows_dev, :] += dot_parts(split(anom, 3), [s1_ref[p, :, at] for p in range(3)], 1)

    invert_in_place(c_ref, panel_ref, swept_ref, trans_ref, cross1)
    innov1 = split(value_ref[:, 1:2] - mean_ref[obs1:obs0, :], 2)
    t_ref[:rows_dev, :] = t_ref[:rows_dev, :] * (rho_ref[1] * -scale)
    for p, part in enumerate(split(c_ref[...], 3)):
        v_ref[p] = part
    gain1 = gain(slice(0, rows_dev), 2)
    mean = mean_ref[:rows_dev, :] + dot_parts(gain1, innov1, 0)
    copies = []
    for i in range(members // wide):
        at = slice(i * wide, (i + 1) * wide)
        change = dot_parts(gain1, [s1_ref[p, :, at] for p in range(2)], 0)
        stage_ref[:, at] = jnp.concatenate([mean] * 2, axis=1) + q_ref[:rows_dev, at] - 0.5 * change
        for side in range(2):
            j = 2 * i + side
            copies.append(
                pltpu.make_async_copy(
                    stage_ref.at[:, 128 * j : 128 * j + 128], out_ref.at[:, member_chunk(i, side)], sems.at[j]
                )
            )
            copies[-1].start()
    for copy in copies:
        copy.wait()


def on_core(kernel, name, outs, smem, vmem, scratch=(), limit_mib=6):
    return pl.pallas_call(
        kernel,
        out_shape=outs,
        in_specs=[pl.BlockSpec(memory_space=SMEM)] * len(smem) + [pl.BlockSpec(memory_space=VMEM)] * len(vmem),
        out_specs=jax.tree.map(lambda _: pl.BlockSpec(memory_space=VMEM), outs),
        scratch_shapes=list(scratch),
        compiler_params=pltpu.CompilerParams(vmem_limit_bytes=limit_mib and limit_mib * 1024 * 1024),
        name=name,
    )(*smem, *vmem)


def exchange(x, axis, groups=None):
    return lax.all_to_all(x, axis, split_axis=0, concat_axis=0, axis_index_groups=groups, tiled=True)


def floats(*shape):
    return jax.ShapeDtypeStruct(shape, jnp.float32)


def prepare(place, owner, taper_mask, ensemble, obs_rows, obs_value, obs_var, ncols, local_len):
    rows_dev, members = ensemble.shape
    n = obs_rows.shape[1]
    return on_core(
        functools.partial(prepare_kernel, ncols=ncols, local_len=local_len), "prepare",
        (floats(2, rows_dev, n), floats(n, n), floats(rows_dev, members), floats(rows_dev, 128),
         floats(n, 128), floats(2, n)),
        (place, owner, taper_mask), (ensemble, obs_rows, obs_rows.T, obs_value.T, obs_var),
    )


def assimilate(place, own, other, kept, prepared):
    rows_dev, members = prepared[2].shape
    n = prepared[1].shape[0]
    total = rows_dev + 2 * n
    return pl.pallas_call(
        assimilate_kernel,
        out_shape=floats(rows_dev, members),
        in_specs=[pl.BlockSpec(memory_space=SMEM)] + [pl.BlockSpec(memory_space=VMEM)] * (3 + len(prepared)),
        out_specs=pl.BlockSpec(memory_space=pl.ANY),
        scratch_shapes=[
            VMEM((rows_dev + n, members), jnp.float32),
            VMEM((3, n, members), jnp.bfloat16),
            VMEM((3, n, members), jnp.bfloat16),
            VMEM((rows_dev + n, n), jnp.float32),
            VMEM((n, n), jnp.float32),
            VMEM((3, rows_dev + n, n), jnp.bfloat16),
            VMEM((total, 128), jnp.float32),
            VMEM((PIVOTS, n), jnp.float32),
            VMEM((2, PIVOTS, n), jnp.float32),
            VMEM((2, n, len(TERMS) * PIVOTS), jnp.bfloat16),
            VMEM((3, n, n), jnp.bfloat16),
            VMEM((3, n, 128), jnp.bfloat16),
            VMEM((rows_dev, members), jnp.float32),
            pltpu.SemaphoreType.DMA((members // 128,)),
        ],
        compiler_params=pltpu.CompilerParams(vmem_limit_bytes=40 * 1024 * 1024),
        name="assimilate",
    )(place, own, other, kept, *prepared)


def on_device(ensemble, obs_rows, owner, obs_value, obs_var, taper_mask):
    rows, members = ensemble.shape
    ncols, nrows = lax.axis_size("col"), lax.axis_size("row")
    my_row, my_col = lax.axis_index("row"), lax.axis_index("col")
    per_dev = obs_rows.shape[1] // ncols
    picked = on_core(
        pick_kernel, "pick_rows", floats(nrows, 1, 1024 + 128),
        (obs_rows, my_col[None], taper_mask), (ensemble,), [VMEM((2 * per_dev, members), jnp.float32)], None,
    )
    pieces = exchange(picked, "row")
    place = jnp.stack([my_row % 2, (my_row * ncols + my_col) * rows]).astype(jnp.int32)
    source = jnp.stack([jnp.where(my_row < nrows // 2, owner[0], owner[1]), owner[1]])
    prepared = prepare(place, owner, taper_mask, ensemble, obs_rows, obs_value, obs_var, ncols, rows * nrows * ncols // 4)
    pieces, source, place, *prepared = lax.optimization_barrier((pieces, source, place, *prepared))
    line = exchange(on_core(forward_kernel, "forward", floats(ncols, 1, 1024 + 128), (source,), (pieces,)), "col")
    wide, kept = on_core(
        share_kernel, "share", (floats(nrows // 2, ncols, 8, 128), floats(ncols, 128)),
        (), (line,), [VMEM((ncols, 8, 128), jnp.float32)],
    )
    own = exchange(wide, "row", [[r for r in range(nrows) if r % 2 == c] for c in range(2)])
    other = lax.ppermute(own, "row", [(r, r ^ 1) for r in range(nrows)])
    return assimilate(place, own, other, kept, prepared)


def solution(mesh):
    in_specs = (P(("row", "col"), None), P(), P(), P(), P(), P(None, ("row", "col"), None))
    out_specs = P(("row", "col"), None)
    return jax.shard_map(
        on_device, mesh=mesh, in_specs=in_specs, out_specs=out_specs, check_vma=False
    )
```

```python
import functools

import jax
import jax.numpy as jnp
from jax import lax
from jax.experimental import pallas as pl
from jax.experimental.pallas import tpu as pltpu
from jax.sharding import PartitionSpec as P

VMEM = pltpu.VMEM
SMEM = pltpu.SMEM
PIVOTS = 32
TERMS = ((0, 0), (0, 1), (1, 0), (1, 1), (0, 2), (2, 0))


def split(x, parts):
    out = []
    for i in range(parts):
        out.append(x.astype(jnp.bfloat16))
        if i < parts - 1:
            x = x - out[-1].astype(jnp.float32)
    return out


def dot_parts(a, b, contract):
    pairs = TERMS[: 3 if len(a) == 2 else 6]
    left = jnp.concatenate([a[i] for i, _ in pairs], axis=1)
    right = jnp.concatenate([b[j] for _, j in pairs], axis=contract)
    return lax.dot_general(
        left, right, (((1,), (contract,)), ((), ())), preferred_element_type=jnp.float32
    )


def by_terms(x, side):
    parts = split(x, 3)
    return jnp.concatenate([parts[term[side]] for term in TERMS], axis=0)


def one_pass(a, b):
    return jnp.dot(a, b, preferred_element_type=jnp.float32)


def spread(x, row):
    return jnp.broadcast_to(x[row : row + 1, :], (8, 128))


def sweep_panel(panel, base, lanes, subs):
    high = base >= 128
    q0 = base - jnp.where(high, 128, 0)
    low_half = [panel[8 * g : 8 * g + 8, :128] for g in range(4)]
    high_half = [panel[8 * g : 8 * g + 8, 128:] for g in range(4)]
    act = [jnp.where(high, h, l) for l, h in zip(low_half, high_half)]
    oth = [jnp.where(high, l, h) for l, h in zip(low_half, high_half)]

    def column(g, c):
        return jnp.take_along_axis(act[g], jnp.full((8, 128), q0 + c, jnp.int32), axis=1)

    diag = [column(0, l) for l in range(8)]
    for sb in range(4):
        cols = [[None] * 4 for _ in range(8)]
        later = [g for g in range(sb + 1, 4)] + [g for g in range(sb)]
        for g in later[:1]:
            for l in range(8):
                cols[l][g] = column(g, 8 * sb + l)
        following = [column(sb + 1, 8 * sb + 8 + l) for l in range(8)] if sb < 3 else None
        for g in later[1:]:
            for l in range(8):
                cols[l][g] = column(g, 8 * sb + l)
        invs, factors = [], [[None] * 8 for _ in range(8)]
        for l in range(8):
            at_row = subs == l
            inv = 1.0 / spread(diag[l], l)
            invs.append(inv)
            for m in range(l + 1, 8):
                t = spread(diag[m], l) * inv
                factors[l][m] = t
                diag[m] = jnp.where(at_row, t, diag[m] - diag[l] * t)
        for l in range(8):
            cols[l][sb] = diag[l]
        for g in later:
            for l in range(8):
                for m in range(l + 1, 8):
                    cols[m][g] = cols[m][g] - cols[l][g] * factors[l][m]
        if sb < 3:
            for l in range(8):
                scaled = cols[l][sb + 1] * invs[l]
                following = [f - cols[l][sb + 1] * spread(scaled, m) for m, f in enumerate(following)]
        for l in range(8):
            u = cols[l]
            at_row = subs == l
            at_lane = lanes == q0 + (8 * sb + l)
            inv = invs[l]
            row_act = jnp.where(at_lane, -inv, spread(act[sb], l) * inv)
            row_oth = spread(oth[sb], l) * inv
            act = [jnp.where(at_lane, 0.0, act[g]) - u[g] * row_act for g in range(4)]
            oth = [oth[g] - u[g] * row_oth for g in range(4)]
            act[sb] = jnp.where(at_row, row_act, act[sb])
            oth[sb] = jnp.where(at_row, row_oth, oth[sb])
        diag = following
    act, oth = jnp.concatenate(act, 0), jnp.concatenate(oth, 0)
    return jnp.concatenate(
        [jnp.where(high, oth, act), jnp.where(high, act, oth)], axis=1
    )


def invert_in_place(a_ref, panel_ref, swept_ref, trans_ref, beside):
    n = a_ref.shape[0]
    steps = n // PIVOTS
    lanes = lax.broadcasted_iota(jnp.int32, (8, 128), 1)
    subs = lax.broadcasted_iota(jnp.int32, (8, 128), 0)
    columns = lax.broadcasted_iota(jnp.int32, (n, n), 1)

    def inside(k, rows):
        return (columns[:rows] >= k * PIVOTS) & (columns[:rows] < (k + 1) * PIVOTS)

    def rows_of(k):
        return pl.ds(pl.multiple_of(k * PIVOTS, PIVOTS), PIVOTS)

    def apply(k, slot):
        a_ref[...] = jnp.where(inside(k, n), 0.0, a_ref[...]) - one_pass(
            trans_ref[slot], by_terms(swept_ref[slot], 1)
        )

    panel_ref[...] = a_ref[:PIVOTS, :]
    swept_ref[1] = jnp.zeros_like(panel_ref)
    trans_ref[1] = jnp.zeros(trans_ref.shape[1:], jnp.bfloat16)

    def step(k, carry):
        now, before = k % 2, (k + 1) % 2
        panel = panel_ref[...]
        trans_ref[now] = by_terms(panel, 0).T
        swept = sweep_panel(panel, k * PIVOTS, lanes, subs)
        apply(k - 1, before)
        last = jnp.maximum(k - 1, 0)
        a_ref[rows_of(last), :] = jnp.where(k > 0, swept_ref[before], a_ref[rows_of(last), :])
        beside(k)
        following = jnp.minimum(k + 1, steps - 1)
        panel_ref[...] = jnp.where(inside(k, PIVOTS), 0.0, a_ref[rows_of(following), :]) - one_pass(
            trans_ref[now, rows_of(following), :], by_terms(swept, 1)
        )
        swept_ref[now] = swept
        return carry

    lax.fori_loop(0, steps, step, 0)
    final = (steps - 1) % 2
    apply(steps - 1, final)
    a_ref[n - PIVOTS :, :] = swept_ref[final]


def pick_kernel(rows_ref, col_ref, mask_ref, x_ref, out_ref, held):
    members = x_ref.shape[1]
    per_dev = held.shape[0] // 2
    start = col_ref[0] * per_dev
    for b in range(2):
        for i in range(per_dev):
            r = rows_ref[b, start + i]
            held[b * per_dev + i : b * per_dev + i + 1, :] = x_ref[pl.ds(r, 1), :]
    chunks = members // 128
    lanes = lax.broadcasted_iota(jnp.int32, (1, 128), 1)
    kept = jnp.where(lanes == 0, mask_ref[0, 0, 0], mask_ref[0, 0, 1]).astype(jnp.float32)
    for piece in range(out_ref.shape[0]):
        g, j = piece // chunks, piece % chunks
        for s in range(8):
            out_ref[piece, :, 128 * s : 128 * s + 128] = held[8 * g + s : 8 * g + s + 1, 128 * j : 128 * j + 128]
        out_ref[piece, :, 1024:] = kept


def share_kernel(line_ref, out_ref, kept_ref, held):
    for c in range(line_ref.shape[0]):
        for s in range(8):
            held[c, s : s + 1, :] = line_ref[c, :, 128 * s : 128 * s + 128]
        kept_ref[c : c + 1, :] = line_ref[c, :, 1024:]
    for d in range(out_ref.shape[0]):
        out_ref[d] = held[...]


def prepare_kernel(
    first_ref, owner_ref, mask_ref, x_ref, rows_ref, given_ref, var_ref,
    rho_ref, decay_ref, anom_ref, mean_ref, value_ref, held_var_ref, *, ncols, local_len,
):
    rows_dev, members = x_ref.shape
    n = rows_ref.shape[1]
    per_dev = n // ncols
    lane = lax.broadcasted_iota(jnp.int32, (1, n), 1)
    here = first_ref[0] + lax.broadcasted_iota(jnp.int32, (rows_dev, 1), 0)
    sub = lax.broadcasted_iota(jnp.int32, (n, 1), 0)
    diag = lax.broadcasted_iota(jnp.int32, (n, n), 0) == lax.broadcasted_iota(jnp.int32, (n, n), 1)

    def column(row):
        return jnp.sum(jnp.where(diag, row, 0.0), axis=1, keepdims=True)

    seen = column(rows_ref[1:2, :].astype(jnp.float32)).astype(jnp.int32)
    there = (owner_ref[1] * ncols + sub // per_dev) * rows_dev + seen

    def decay(positions, b):
        glob = (owner_ref[b] * ncols + lane // per_dev) * rows_dev + rows_ref[b : b + 1, :]
        dist = jnp.abs(positions - glob).astype(jnp.float32)
        return jnp.exp(-dist / jnp.float32(local_len))

    for b in range(2):
        mask = jnp.where(lane < 128, mask_ref[b, 0, 0], mask_ref[b, 0, 1]).astype(jnp.float32)
        rho_ref[b] = decay(here, b) * mask
    decay_ref[...] = decay(there, 0)
    x = x_ref[...]
    mean = jnp.sum(x, axis=1, keepdims=True) * (1.0 / members)
    anom_ref[...] = x - mean
    mean_ref[...] = jnp.broadcast_to(mean, mean_ref.shape)
    held = lax.broadcasted_iota(jnp.int32, value_ref.shape, 1)
    value_ref[...] = jnp.where(held == 0, column(given_ref[0:1, :]), column(given_ref[1:2, :]))
    held_var_ref[...] = var_ref[...]


def assimilate_kernel(
    core_ref, own_ref, other_ref, kept_ref, rho_ref, decay_ref, x_ref, x_mean_ref, value_ref, var_ref,
    out_ref, q_ref, s0_ref, s1_ref, t_ref, c_ref, g_ref, mean_ref, panel_ref, swept_ref, trans_ref,
    v_ref, innov_ref, w_ref, v1_ref, e_ref, stage_ref, sems,
):
    rows_dev, members = x_ref.shape
    n = var_ref.shape[1]
    ncols = kept_ref.shape[0]
    per_dev = n // ncols
    groups = per_dev // 8
    chunks = members // 128
    core = core_ref[0]
    scale = 1.0 / (members - 1.0)
    obs1, obs0 = rows_dev, rows_dev + n

    def member_chunk(i, side):
        return pl.ds(pl.multiple_of((2 * i + (core if side == 0 else 1 - core)) * 128, 128), 128)

    def chunk(j, width):
        return pl.ds(pl.multiple_of(j * width, width), width)

    def observed(b, i, ref):
        return jnp.concatenate(
            [ref[(b * groups + g) * (chunks // 2) + i, c] for c in range(ncols) for g in range(groups)], axis=0
        )

    def add_up(c, carry):
        for b, top in ((0, obs0), (1, obs1)):
            for g in range(groups):
                slots = [(b * groups + g) * (chunks // 2) + i for i in range(chunks // 2)]
                total = own_ref[slots[0], c] + other_ref[slots[0], c]
                for slot in slots[1:]:
                    total = total + (own_ref[slot, c] + other_ref[slot, c])
                mean_ref[pl.ds(pl.multiple_of(top + c * per_dev + g * 8, 8), 8), :] = total
        return carry

    lax.fori_loop(0, ncols, add_up, 0)
    mean = jnp.sum(mean_ref[obs1:, :], axis=1, keepdims=True) * (1.0 / members)
    mean_ref[obs1:, :] = jnp.broadcast_to(mean, (2 * n, 128))
    mean_ref[:rows_dev, :] = x_mean_ref[...]

    wide = 2 * 128
    diag = lax.broadcasted_iota(jnp.int32, (n, n), 0) == lax.broadcasted_iota(jnp.int32, (n, n), 1)
    c_ref[...] = jnp.zeros_like(c_ref)

    def covariance0(i, carry):
        mean = mean_ref[obs0:, :]
        anom = jnp.concatenate([observed(0, i, own_ref) - mean, observed(0, i, other_ref) - mean], axis=1)
        parts = split(anom, 3)
        for p in range(3):
            s0_ref[p, :, chunk(i, wide)] = parts[p]
        c_ref[...] += dot_parts(parts, parts, 1)
        return carry

    lax.fori_loop(0, members // wide, covariance0, 0)
    for p, part in enumerate(split(c_ref[...], 3)):
        w_ref[p] = part
    c_ref[...] = c_ref[...] * scale + jnp.where(diag, var_ref[0:1, :], 0.0)
    t_ref[...] = jnp.zeros_like(t_ref)
    e_ref[...] = jnp.zeros_like(e_ref)

    def cross0(j):
        at, i, side = chunk(j, 128), j // 2, j % 2
        local = jnp.where(side == 0, x_ref[:, member_chunk(i, 0)], x_ref[:, member_chunk(i, 1)])
        seen = jnp.where(side == 0, observed(1, i, own_ref), observed(1, i, other_ref))
        for top, anom in ((0, local), (obs1, seen - mean_ref[obs1:obs0, :])):
            rows = slice(top, top + anom.shape[0])
            q_ref[rows, at] = anom
            parts = split(anom, 3)
            t_ref[rows, :] += dot_parts(parts, [s0_ref[p, :, at] for p in range(3)], 1)
            if top:
                e_ref[...] += dot_parts(parts, parts, 1)

    invert_in_place(c_ref, panel_ref, swept_ref, trans_ref, cross0)

    for p, part in enumerate(split(c_ref[...], 3)):
        v_ref[p] = part

    def gain(tapered, parts):
        return split(dot_parts(split(tapered, 3), [v_ref[p] for p in range(3)], 0), parts)

    for half in range(2):
        kept = jnp.concatenate(
            [
                jnp.concatenate(
                    [jnp.broadcast_to(kept_ref[c : c + 1, i : i + 1] * -scale, (per_dev, 128)) for i in range(2)],
                    axis=1,
                )
                for c in range(half * ncols // 2, (half + 1) * ncols // 2)
            ],
            axis=0,
        )
        rows = slice(half * n // 2, (half + 1) * n // 2)
        at = slice(obs1 + half * n // 2, obs1 + (half + 1) * n // 2)
        for p, part in enumerate(gain(t_ref[at, :] * (decay_ref[rows, :] * kept), 3)):
            g_ref[p, at, :] = part

    for half in range(2):
        at = slice(obs1 + half * n // 2, obs1 + (half + 1) * n // 2)
        product = dot_parts([g_ref[p, at, :] for p in range(3)], [w_ref[p] for p in range(3)], 0)
        for p, part in enumerate(split(0.25 * product - t_ref[at, :], 3)):
            v1_ref[p, half * n // 2 : (half + 1) * n // 2, :] = part
    for half in range(2):
        at = slice(obs1 + half * n // 2, obs1 + (half + 1) * n // 2)
        c_ref[half * n // 2 : (half + 1) * n // 2, :] = dot_parts(
            [g_ref[p, at, :] for p in range(3)], [v1_ref[p] for p in range(3)], 1
        )
    c_ref[...] = (e_ref[...] + 0.5 * (c_ref[...] + c_ref[...].T)) * scale + jnp.where(diag, var_ref[1:2, :], 0.0)

    for p, part in enumerate(gain(t_ref[:rows_dev, :] * (rho_ref[0] * -scale), 2)):
        g_ref[p, :rows_dev, :] = part
    for p, part in enumerate(split(value_ref[:, 0:1] - mean_ref[obs0:, :], 3)):
        innov_ref[p] = part
    t_ref[:rows_dev, :] = jnp.zeros((rows_dev, n), jnp.float32)

    def cross1(j):
        at = chunk(j, 128)
        some = pl.ds(pl.multiple_of(obs1 + j * (n // chunks), n // chunks), n // chunks)
        mean_ref[some, :] += dot_parts(
            [g_ref[p, some, :] for p in range(3)], [innov_ref[p] for p in range(3)], 0
        )
        some = chunk(j, rows_dev // chunks)
        mean_ref[some, :] += dot_parts(
            [g_ref[p, some, :] for p in range(2)], [innov_ref[p] for p in range(2)], 0
        )
        change = dot_parts(
            [g_ref[p, obs1:obs0, :] for p in range(3)], [s0_ref[p, :, at] for p in range(3)], 0
        )
        seen = split(q_ref[obs1:obs0, at] - 0.5 * change, 3)
        for p in range(3):
            s1_ref[p, :, at] = seen[p]
        change = dot_parts(
            [g_ref[p, :rows_dev, :] for p in range(2)], [s0_ref[p, :, at] for p in range(2)], 0
        )
        anom = q_ref[:rows_dev, at] - 0.5 * change
        q_ref[:rows_dev, at] = anom
        t_ref[:rows_dev, :] += dot_parts(split(anom, 3), seen, 1)

    invert_in_place(c_ref, panel_ref, swept_ref, trans_ref, cross1)
    innov1 = split(value_ref[:, 1:2] - mean_ref[obs1:obs0, :], 2)
    for p, part in enumerate(split(c_ref[...], 3)):
        v_ref[p] = part
    gain1 = gain(t_ref[:rows_dev, :] * (rho_ref[1] * -scale), 2)
    mean = mean_ref[:rows_dev, :] + dot_parts(gain1, innov1, 0)
    copies = []
    for i in range(members // wide):
        at = slice(i * wide, (i + 1) * wide)
        change = dot_parts(gain1, [s1_ref[p, :, at] for p in range(2)], 0)
        stage_ref[:, at] = jnp.concatenate([mean] * 2, axis=1) + q_ref[:rows_dev, at] - 0.5 * change
        for side in range(2):
            j = 2 * i + side
            copies.append(
                pltpu.make_async_copy(
                    stage_ref.at[:, 128 * j : 128 * j + 128], out_ref.at[:, member_chunk(i, side)], sems.at[j]
                )
            )
            copies[-1].start()
    for copy in copies:
        copy.wait()


def on_core(kernel, name, outs, smem, vmem, scratch=(), limit_mib=6):
    return pl.pallas_call(
        kernel,
        out_shape=outs,
        in_specs=[pl.BlockSpec(memory_space=SMEM)] * len(smem) + [pl.BlockSpec(memory_space=VMEM)] * len(vmem),
        out_specs=jax.tree.map(lambda _: pl.BlockSpec(memory_space=VMEM), outs),
        scratch_shapes=list(scratch),
        compiler_params=pltpu.CompilerParams(vmem_limit_bytes=limit_mib and limit_mib * 1024 * 1024),
        name=name,
    )(*smem, *vmem)


def exchange(x, axis, groups=None):
    return lax.all_to_all(x, axis, split_axis=0, concat_axis=0, axis_index_groups=groups, tiled=True)


def floats(*shape):
    return jax.ShapeDtypeStruct(shape, jnp.float32)


def prepare(first, owner, taper_mask, ensemble, obs_rows, obs_value, obs_var, ncols, local_len):
    rows_dev, members = ensemble.shape
    n = obs_rows.shape[1]
    return on_core(
        functools.partial(prepare_kernel, ncols=ncols, local_len=local_len), "prepare",
        (floats(2, rows_dev, n), floats(n, n), floats(rows_dev, members), floats(rows_dev, 128),
         floats(n, 128), floats(2, n)),
        (first, owner, taper_mask), (ensemble, obs_rows, obs_value, obs_var), limit_mib=None,
    )


def assimilate(core, own, other, kept, prepared):
    rows_dev, members = prepared[2].shape
    n = prepared[1].shape[0]
    total = rows_dev + 2 * n
    return pl.pallas_call(
        assimilate_kernel,
        out_shape=floats(rows_dev, members),
        in_specs=[pl.BlockSpec(memory_space=SMEM)] + [pl.BlockSpec(memory_space=VMEM)] * (3 + len(prepared)),
        out_specs=pl.BlockSpec(memory_space=pl.ANY),
        scratch_shapes=[
            VMEM((rows_dev + n, members), jnp.float32),
            VMEM((3, n, members), jnp.bfloat16),
            VMEM((3, n, members), jnp.bfloat16),
            VMEM((rows_dev + n, n), jnp.float32),
            VMEM((n, n), jnp.float32),
            VMEM((3, rows_dev + n, n), jnp.bfloat16),
            VMEM((total, 128), jnp.float32),
            VMEM((PIVOTS, n), jnp.float32),
            VMEM((2, PIVOTS, n), jnp.float32),
            VMEM((2, n, len(TERMS) * PIVOTS), jnp.bfloat16),
            VMEM((3, n, n), jnp.bfloat16),
            VMEM((3, n, 128), jnp.bfloat16),
            VMEM((3, n, n), jnp.bfloat16),
            VMEM((3, n, n), jnp.bfloat16),
            VMEM((n, n), jnp.float32),
            VMEM((rows_dev, members), jnp.float32),
            pltpu.SemaphoreType.DMA((members // 128,)),
        ],
        compiler_params=pltpu.CompilerParams(vmem_limit_bytes=40 * 1024 * 1024),
        name="assimilate",
    )(core, own, other, kept, *prepared)


def on_device(ensemble, obs_rows, owner, obs_value, obs_var, taper_mask):
    rows, members = ensemble.shape
    ncols, nrows = lax.axis_size("col"), lax.axis_size("row")
    my_row, my_col = lax.axis_index("row"), lax.axis_index("col")
    per_dev = obs_rows.shape[1] // ncols
    picked = on_core(
        pick_kernel, "pick_rows", floats(nrows, 1, 1024 + 128),
        (obs_rows, my_col[None], taper_mask), (ensemble,), [VMEM((2 * per_dev, members), jnp.float32)], None,
    )
    pieces = exchange(picked, "row")
    first, core = ((my_row * ncols + my_col) * rows)[None], (my_row & 1)[None]
    prepared = prepare(first, owner, taper_mask, ensemble, obs_rows, obs_value, obs_var, ncols, rows * nrows * ncols // 4)
    source = jnp.where(my_row < nrows // 2, owner[0], owner[1])
    source, seen, pieces, *prepared = lax.optimization_barrier((source, owner[1], pieces, *prepared))
    tile = lax.dynamic_index_in_dim(pieces, source, 0)[:, :, :1024]
    mask = lax.dynamic_index_in_dim(pieces, seen, 0)[:, :, 1024:]
    line = jnp.broadcast_to(jnp.concatenate([tile, mask], axis=2), (ncols, 1, 1024 + 128))
    line = exchange(line, "col")
    wide, kept = on_core(
        share_kernel, "share", (floats(nrows // 2, ncols, 8, 128), floats(ncols, 128)),
        (), (line,), [VMEM((ncols, 8, 128), jnp.float32)],
    )
    own = exchange(wide, "row", [[r for r in range(nrows) if r % 2 == c] for c in range(2)])
    other = lax.ppermute(own, "row", [(r, r ^ 1) for r in range(nrows)])
    return assimilate(core, own, other, kept, prepared)


def solution(mesh):
    in_specs = (P(("row", "col"), None), P(), P(), P(), P(), P(None, ("row", "col"), None))
    out_specs = P(("row", "col"), None)
    return jax.shard_map(
        on_device, mesh=mesh, in_specs=in_specs, out_specs=out_specs, check_vma=False
    )
```

```python
import functools

import jax
import jax.numpy as jnp
from jax import lax
from jax.experimental import pallas as pl
from jax.experimental.pallas import tpu as pltpu
from jax.sharding import PartitionSpec as P

VMEM = pltpu.VMEM
SMEM = pltpu.SMEM
PIVOTS = 32
TERMS = ((0, 0), (0, 1), (1, 0), (1, 1), (0, 2), (2, 0))


def split(x, parts):
    out = []
    for i in range(parts):
        out.append(x.astype(jnp.bfloat16))
        if i < parts - 1:
            x = x - out[-1].astype(jnp.float32)
    return out


def dot_parts(a, b, contract):
    pairs = TERMS[: 3 if len(a) == 2 else 6]
    left = jnp.concatenate([a[i] for i, _ in pairs], axis=1)
    right = jnp.concatenate([b[j] for _, j in pairs], axis=contract)
    return lax.dot_general(
        left, right, (((1,), (contract,)), ((), ())), preferred_element_type=jnp.float32
    )


def by_terms(x, side):
    parts = split(x, 3)
    return jnp.concatenate([parts[term[side]] for term in TERMS], axis=0)


def one_pass(a, b):
    return jnp.dot(a, b, preferred_element_type=jnp.float32)


def spread(x, row):
    return jnp.broadcast_to(x[row : row + 1, :], (8, 128))


def sweep_panel(panel, base, lanes, subs):
    high = base >= 128
    q0 = base - jnp.where(high, 128, 0)
    low_half = [panel[8 * g : 8 * g + 8, :128] for g in range(4)]
    high_half = [panel[8 * g : 8 * g + 8, 128:] for g in range(4)]
    act = [jnp.where(high, h, l) for l, h in zip(low_half, high_half)]
    oth = [jnp.where(high, l, h) for l, h in zip(low_half, high_half)]

    def column(g, c):
        return jnp.take_along_axis(act[g], jnp.full((8, 128), q0 + c, jnp.int32), axis=1)

    diag = [column(0, l) for l in range(8)]
    for sb in range(4):
        cols = [[None] * 4 for _ in range(8)]
        later = [g for g in range(sb + 1, 4)] + [g for g in range(sb)]
        for g in later[:1]:
            for l in range(8):
                cols[l][g] = column(g, 8 * sb + l)
        following = [column(sb + 1, 8 * sb + 8 + l) for l in range(8)] if sb < 3 else None
        for g in later[1:]:
            for l in range(8):
                cols[l][g] = column(g, 8 * sb + l)
        invs, factors = [], [[None] * 8 for _ in range(8)]
        for l in range(8):
            at_row = subs == l
            inv = 1.0 / spread(diag[l], l)
            invs.append(inv)
            for m in range(l + 1, 8):
                t = spread(diag[m], l) * inv
                factors[l][m] = t
                diag[m] = jnp.where(at_row, t, diag[m] - diag[l] * t)
        for l in range(8):
            cols[l][sb] = diag[l]
        for g in later:
            for l in range(8):
                for m in range(l + 1, 8):
                    cols[m][g] = cols[m][g] - cols[l][g] * factors[l][m]
        if sb < 3:
            for l in range(8):
                scaled = cols[l][sb + 1] * invs[l]
                following = [f - cols[l][sb + 1] * spread(scaled, m) for m, f in enumerate(following)]
        for l in range(8):
            u = cols[l]
            at_row = subs == l
            at_lane = lanes == q0 + (8 * sb + l)
            inv = invs[l]
            row_act = jnp.where(at_lane, -inv, spread(act[sb], l) * inv)
            row_oth = spread(oth[sb], l) * inv
            act = [jnp.where(at_lane, 0.0, act[g]) - u[g] * row_act for g in range(4)]
            oth = [oth[g] - u[g] * row_oth for g in range(4)]
            act[sb] = jnp.where(at_row, row_act, act[sb])
            oth[sb] = jnp.where(at_row, row_oth, oth[sb])
        diag = following
    act, oth = jnp.concatenate(act, 0), jnp.concatenate(oth, 0)
    return jnp.concatenate(
        [jnp.where(high, oth, act), jnp.where(high, act, oth)], axis=1
    )


def invert_in_place(a_ref, panel_ref, swept_ref, trans_ref, beside):
    n = a_ref.shape[0]
    steps = n // PIVOTS
    lanes = lax.broadcasted_iota(jnp.int32, (8, 128), 1)
    subs = lax.broadcasted_iota(jnp.int32, (8, 128), 0)
    columns = lax.broadcasted_iota(jnp.int32, (n, n), 1)

    def inside(k, rows):
        return (columns[:rows] >= k * PIVOTS) & (columns[:rows] < (k + 1) * PIVOTS)

    def rows_of(k):
        return pl.ds(pl.multiple_of(k * PIVOTS, PIVOTS), PIVOTS)

    def apply(k, slot):
        a_ref[...] = jnp.where(inside(k, n), 0.0, a_ref[...]) - one_pass(
            trans_ref[slot], by_terms(swept_ref[slot], 1)
        )

    panel_ref[...] = a_ref[:PIVOTS, :]
    swept_ref[1] = jnp.zeros_like(panel_ref)
    trans_ref[1] = jnp.zeros(trans_ref.shape[1:], jnp.bfloat16)

    def step(k, carry):
        now, before = k % 2, (k + 1) % 2
        panel = panel_ref[...]
        trans_ref[now] = by_terms(panel, 0).T
        swept = sweep_panel(panel, k * PIVOTS, lanes, subs)
        apply(k - 1, before)
        last = jnp.maximum(k - 1, 0)
        a_ref[rows_of(last), :] = jnp.where(k > 0, swept_ref[before], a_ref[rows_of(last), :])
        beside(k)
        following = jnp.minimum(k + 1, steps - 1)
        panel_ref[...] = jnp.where(inside(k, PIVOTS), 0.0, a_ref[rows_of(following), :]) - one_pass(
            trans_ref[now, rows_of(following), :], by_terms(swept, 1)
        )
        swept_ref[now] = swept
        return carry

    lax.fori_loop(0, steps, step, 0)
    final = (steps - 1) % 2
    apply(steps - 1, final)
    a_ref[n - PIVOTS :, :] = swept_ref[final]


def pick_kernel(rows_ref, col_ref, mask_ref, x_ref, out_ref, held):
    members = x_ref.shape[1]
    per_dev = held.shape[0] // 2
    start = col_ref[0] * per_dev
    for b in range(2):
        for i in range(per_dev):
            r = rows_ref[b, start + i]
            held[b * per_dev + i : b * per_dev + i + 1, :] = x_ref[pl.ds(r, 1), :]
    chunks = members // 128
    lanes = lax.broadcasted_iota(jnp.int32, (1, 128), 1)
    kept = jnp.where(lanes == 0, mask_ref[0, 0, 0], mask_ref[0, 0, 1]).astype(jnp.float32)
    for piece in range(out_ref.shape[0]):
        g, j = piece // chunks, piece % chunks
        for s in range(8):
            out_ref[piece, :, 128 * s : 128 * s + 128] = held[8 * g + s : 8 * g + s + 1, 128 * j : 128 * j + 128]
        out_ref[piece, :, 1024:] = kept


def share_kernel(line_ref, out_ref, kept_ref, held):
    for c in range(line_ref.shape[0]):
        for s in range(8):
            held[c, s : s + 1, :] = line_ref[c, :, 128 * s : 128 * s + 128]
        kept_ref[c : c + 1, :] = line_ref[c, :, 1024:]
    for d in range(out_ref.shape[0]):
        out_ref[d] = held[...]


def prepare_kernel(
    first_ref, owner_ref, mask_ref, x_ref, rows_ref, given_ref, var_ref,
    rho_ref, decay_ref, anom_ref, mean_ref, value_ref, held_var_ref, *, ncols, local_len,
):
    rows_dev, members = x_ref.shape
    n = rows_ref.shape[1]
    per_dev = n // ncols
    lane = lax.broadcasted_iota(jnp.int32, (1, n), 1)
    here = first_ref[0] + lax.broadcasted_iota(jnp.int32, (rows_dev, 1), 0)
    sub = lax.broadcasted_iota(jnp.int32, (n, 1), 0)
    diag = lax.broadcasted_iota(jnp.int32, (n, n), 0) == lax.broadcasted_iota(jnp.int32, (n, n), 1)

    def column(row):
        return jnp.sum(jnp.where(diag, row, 0.0), axis=1, keepdims=True)

    seen = column(rows_ref[1:2, :].astype(jnp.float32)).astype(jnp.int32)
    there = (owner_ref[1] * ncols + sub // per_dev) * rows_dev + seen

    def decay(positions, b):
        glob = (owner_ref[b] * ncols + lane // per_dev) * rows_dev + rows_ref[b : b + 1, :]
        dist = jnp.abs(positions - glob).astype(jnp.float32)
        return jnp.exp(-dist / jnp.float32(local_len))

    for b in range(2):
        mask = jnp.where(lane < 128, mask_ref[b, 0, 0], mask_ref[b, 0, 1]).astype(jnp.float32)
        rho_ref[b] = decay(here, b) * mask
    decay_ref[...] = decay(there, 0)
    x = x_ref[...]
    mean = jnp.sum(x, axis=1, keepdims=True) * (1.0 / members)
    anom_ref[...] = x - mean
    mean_ref[...] = jnp.broadcast_to(mean, mean_ref.shape)
    held = lax.broadcasted_iota(jnp.int32, value_ref.shape, 1)
    value_ref[...] = jnp.where(held == 0, column(given_ref[0:1, :]), column(given_ref[1:2, :]))
    held_var_ref[...] = var_ref[...]


def assimilate_kernel(
    core_ref, own_ref, other_ref, kept_ref, rho_ref, decay_ref, x_ref, x_mean_ref, value_ref, var_ref,
    out_ref, q_ref, s0_ref, s1_ref, t_ref, c_ref, g_ref, mean_ref, panel_ref, swept_ref, trans_ref,
    v_ref, innov_ref, w_ref, v1_ref, e_ref, stage_ref, sems,
):
    rows_dev, members = x_ref.shape
    n = var_ref.shape[1]
    ncols = kept_ref.shape[0]
    per_dev = n // ncols
    groups = per_dev // 8
    chunks = members // 128
    core = core_ref[0]
    scale = 1.0 / (members - 1.0)
    obs1, obs0 = rows_dev, rows_dev + n

    def member_chunk(i, side):
        return pl.ds(pl.multiple_of((2 * i + (core if side == 0 else 1 - core)) * 128, 128), 128)

    def chunk(j, width):
        return pl.ds(pl.multiple_of(j * width, width), width)

    def observed(b, i, ref):
        return jnp.concatenate(
            [ref[(b * groups + g) * (chunks // 2) + i, c] for c in range(ncols) for g in range(groups)], axis=0
        )

    def add_up(c, carry):
        for b, top in ((0, obs0), (1, obs1)):
            for g in range(groups):
                slots = [(b * groups + g) * (chunks // 2) + i for i in range(chunks // 2)]
                total = own_ref[slots[0], c] + other_ref[slots[0], c]
                for slot in slots[1:]:
                    total = total + (own_ref[slot, c] + other_ref[slot, c])
                mean_ref[pl.ds(pl.multiple_of(top + c * per_dev + g * 8, 8), 8), :] = total
        return carry

    lax.fori_loop(0, ncols, add_up, 0)
    mean = jnp.sum(mean_ref[obs1:, :], axis=1, keepdims=True) * (1.0 / members)
    mean_ref[obs1:, :] = jnp.broadcast_to(mean, (2 * n, 128))
    mean_ref[:rows_dev, :] = x_mean_ref[...]

    wide = 2 * 128
    diag = lax.broadcasted_iota(jnp.int32, (n, n), 0) == lax.broadcasted_iota(jnp.int32, (n, n), 1)
    c_ref[...] = jnp.zeros_like(c_ref)

    def covariance0(i, carry):
        mean = mean_ref[obs0:, :]
        anom = jnp.concatenate([observed(0, i, own_ref) - mean, observed(0, i, other_ref) - mean], axis=1)
        parts = split(anom, 3)
        for p in range(3):
            s0_ref[p, :, chunk(i, wide)] = parts[p]
        c_ref[...] += dot_parts(parts, parts, 1)
        return carry

    lax.fori_loop(0, members // wide, covariance0, 0)
    for p, part in enumerate(split(c_ref[...], 3)):
        w_ref[p] = part
    c_ref[...] = c_ref[...] * scale + jnp.where(diag, var_ref[0:1, :], 0.0)
    t_ref[...] = jnp.zeros_like(t_ref)
    e_ref[...] = jnp.zeros_like(e_ref)

    def cross0(j):
        at, i, side = chunk(j, 128), j // 2, j % 2
        local = jnp.where(side == 0, x_ref[:, member_chunk(i, 0)], x_ref[:, member_chunk(i, 1)])
        seen = jnp.where(side == 0, observed(1, i, own_ref), observed(1, i, other_ref))
        for top, anom in ((0, local), (obs1, seen - mean_ref[obs1:obs0, :])):
            rows = slice(top, top + anom.shape[0])
            q_ref[rows, at] = anom
            parts = split(anom, 3)
            t_ref[rows, :] += dot_parts(parts, [s0_ref[p, :, at] for p in range(3)], 1)
            if top:
                e_ref[...] += dot_parts(parts, parts, 1)

    invert_in_place(c_ref, panel_ref, swept_ref, trans_ref, cross0)

    for p, part in enumerate(split(c_ref[...], 3)):
        v_ref[p] = part

    def gain(tapered, parts):
        return split(dot_parts(split(tapered, 3), [v_ref[p] for p in range(3)], 0), parts)

    for half in range(2):
        kept = jnp.concatenate(
            [
                jnp.concatenate(
                    [jnp.broadcast_to(kept_ref[c : c + 1, i : i + 1] * -scale, (per_dev, 128)) for i in range(2)],
                    axis=1,
                )
                for c in range(half * ncols // 2, (half + 1) * ncols // 2)
            ],
            axis=0,
        )
        rows = slice(half * n // 2, (half + 1) * n // 2)
        at = slice(obs1 + half * n // 2, obs1 + (half + 1) * n // 2)
        for p, part in enumerate(gain(t_ref[at, :] * (decay_ref[rows, :] * kept), 3)):
            g_ref[p, at, :] = part

    for half in range(2):
        at = slice(obs1 + half * n // 2, obs1 + (half + 1) * n // 2)
        product = dot_parts([g_ref[p, at, :] for p in range(3)], [w_ref[p] for p in range(3)], 0)
        for p, part in enumerate(split(0.25 * product - t_ref[at, :], 3)):
            v1_ref[p, half * n // 2 : (half + 1) * n // 2, :] = part
    for half in range(2):
        at = slice(obs1 + half * n // 2, obs1 + (half + 1) * n // 2)
        c_ref[half * n // 2 : (half + 1) * n // 2, :] = dot_parts(
            [g_ref[p, at, :] for p in range(3)], [v1_ref[p] for p in range(3)], 1
        )
    c_ref[...] = (e_ref[...] + 0.5 * (c_ref[...] + c_ref[...].T)) * scale + jnp.where(diag, var_ref[1:2, :], 0.0)

    for p, part in enumerate(gain(t_ref[:rows_dev, :] * (rho_ref[0] * -scale), 2)):
        g_ref[p, :rows_dev, :] = part
    for p, part in enumerate(split(value_ref[:, 0:1] - mean_ref[obs0:, :], 3)):
        innov_ref[p] = part
    t_ref[:rows_dev, :] = jnp.zeros((rows_dev, n), jnp.float32)

    def cross1(j):
        at = chunk(j, 128)
        some = pl.ds(pl.multiple_of(obs1 + j * (n // chunks), n // chunks), n // chunks)
        mean_ref[some, :] += dot_parts(
            [g_ref[p, some, :] for p in range(3)], [innov_ref[p] for p in range(3)], 0
        )
        some = chunk(j, rows_dev // chunks)
        mean_ref[some, :] += dot_parts(
            [g_ref[p, some, :] for p in range(2)], [innov_ref[p] for p in range(2)], 0
        )
        change = dot_parts(
            [g_ref[p, obs1:obs0, :] for p in range(3)], [s0_ref[p, :, at] for p in range(3)], 0
        )
        seen = split(q_ref[obs1:obs0, at] - 0.5 * change, 3)
        for p in range(3):
            s1_ref[p, :, at] = seen[p]
        change = dot_parts(
            [g_ref[p, :rows_dev, :] for p in range(2)], [s0_ref[p, :, at] for p in range(2)], 0
        )
        anom = q_ref[:rows_dev, at] - 0.5 * change
        q_ref[:rows_dev, at] = anom
        t_ref[:rows_dev, :] += dot_parts(split(anom, 3), seen, 1)

    invert_in_place(c_ref, panel_ref, swept_ref, trans_ref, cross1)
    innov1 = split(value_ref[:, 1:2] - mean_ref[obs1:obs0, :], 2)
    for p, part in enumerate(split(c_ref[...], 3)):
        v_ref[p] = part
    gain1 = gain(t_ref[:rows_dev, :] * (rho_ref[1] * -scale), 2)
    mean = mean_ref[:rows_dev, :] + dot_parts(gain1, innov1, 0)
    copies = []
    for i in range(members // wide):
        at = slice(i * wide, (i + 1) * wide)
        change = dot_parts(gain1, [s1_ref[p, :, at] for p in range(2)], 0)
        stage_ref[:, at] = jnp.concatenate([mean] * 2, axis=1) + q_ref[:rows_dev, at] - 0.5 * change
        for side in range(2):
            j = 2 * i + side
            copies.append(
                pltpu.make_async_copy(
                    stage_ref.at[:, 128 * j : 128 * j + 128], out_ref.at[:, member_chunk(i, side)], sems.at[j]
                )
            )
            copies[-1].start()
    for copy in copies:
        copy.wait()


def on_core(kernel, name, outs, smem, vmem, scratch=(), limit_mib=6):
    return pl.pallas_call(
        kernel,
        out_shape=outs,
        in_specs=[pl.BlockSpec(memory_space=SMEM)] * len(smem) + [pl.BlockSpec(memory_space=VMEM)] * len(vmem),
        out_specs=jax.tree.map(lambda _: pl.BlockSpec(memory_space=VMEM), outs),
        scratch_shapes=list(scratch),
        compiler_params=pltpu.CompilerParams(vmem_limit_bytes=limit_mib and limit_mib * 1024 * 1024),
        name=name,
    )(*smem, *vmem)


def exchange(x, axis, groups=None):
    return lax.all_to_all(x, axis, split_axis=0, concat_axis=0, axis_index_groups=groups, tiled=True)


def floats(*shape):
    return jax.ShapeDtypeStruct(shape, jnp.float32)


def prepare(first, owner, taper_mask, ensemble, obs_rows, obs_value, obs_var, ncols, local_len):
    rows_dev, members = ensemble.shape
    n = obs_rows.shape[1]
    return on_core(
        functools.partial(prepare_kernel, ncols=ncols, local_len=local_len), "prepare",
        (floats(2, rows_dev, n), floats(n, n), floats(rows_dev, members), floats(rows_dev, 128),
         floats(n, 128), floats(2, n)),
        (first, owner, taper_mask), (ensemble, obs_rows, obs_value, obs_var), limit_mib=None,
    )


def assimilate(core, own, other, kept, prepared):
    rows_dev, members = prepared[2].shape
    n = prepared[1].shape[0]
    total = rows_dev + 2 * n
    return pl.pallas_call(
        assimilate_kernel,
        out_shape=floats(rows_dev, members),
        in_specs=[pl.BlockSpec(memory_space=SMEM)] + [pl.BlockSpec(memory_space=VMEM)] * (3 + len(prepared)),
        out_specs=pl.BlockSpec(memory_space=pl.ANY),
        scratch_shapes=[
            VMEM((rows_dev + n, members), jnp.float32),
            VMEM((3, n, members), jnp.bfloat16),
            VMEM((3, n, members), jnp.bfloat16),
            VMEM((rows_dev + n, n), jnp.float32),
            VMEM((n, n), jnp.float32),
            VMEM((3, rows_dev + n, n), jnp.bfloat16),
            VMEM((total, 128), jnp.float32),
            VMEM((PIVOTS, n), jnp.float32),
            VMEM((2, PIVOTS, n), jnp.float32),
            VMEM((2, n, len(TERMS) * PIVOTS), jnp.bfloat16),
            VMEM((3, n, n), jnp.bfloat16),
            VMEM((3, n, 128), jnp.bfloat16),
            VMEM((3, n, n), jnp.bfloat16),
            VMEM((3, n, n), jnp.bfloat16),
            VMEM((n, n), jnp.float32),
            VMEM((rows_dev, members), jnp.float32),
            pltpu.SemaphoreType.DMA((members // 128,)),
        ],
        compiler_params=pltpu.CompilerParams(vmem_limit_bytes=40 * 1024 * 1024),
        name="assimilate",
    )(core, own, other, kept, *prepared)


def on_device(ensemble, obs_rows, owner, obs_value, obs_var, taper_mask):
    rows, members = ensemble.shape
    ncols, nrows = lax.axis_size("col"), lax.axis_size("row")
    my_row, my_col = lax.axis_index("row"), lax.axis_index("col")
    per_dev = obs_rows.shape[1] // ncols
    picked = on_core(
        pick_kernel, "pick_rows", floats(nrows, 1, 1024 + 128),
        (obs_rows, my_col[None], taper_mask), (ensemble,), [VMEM((2 * per_dev, members), jnp.float32)], None,
    )
    pieces = exchange(picked, "row")
    first, core = ((my_row * ncols + my_col) * rows)[None], (my_row & 1)[None]
    prepared = prepare(first, owner, taper_mask, ensemble, obs_rows, obs_value, obs_var, ncols, rows * nrows * ncols // 4)
    source = jnp.where(my_row < nrows // 2, owner[0], owner[1])
    pieces, *prepared = lax.optimization_barrier((pieces, *prepared))
    tile = lax.dynamic_index_in_dim(pieces, source, 0)[:, :, :1024]
    mask = lax.dynamic_index_in_dim(pieces, owner[1], 0)[:, :, 1024:]
    line = jnp.broadcast_to(jnp.concatenate([tile, mask], axis=2), (ncols, 1, 1024 + 128))
    line = exchange(line, "col")
    wide, kept = on_core(
        share_kernel, "share", (floats(nrows // 2, ncols, 8, 128), floats(ncols, 128)),
        (), (line,), [VMEM((ncols, 8, 128), jnp.float32)],
    )
    own = exchange(wide, "row", [[r for r in range(nrows) if r % 2 == c] for c in range(2)])
    other = lax.ppermute(own, "row", [(r, r ^ 1) for r in range(nrows)])
    return assimilate(core, own, other, kept, prepared)


def solution(mesh):
    in_specs = (P(("row", "col"), None), P(), P(), P(), P(), P(None, ("row", "col"), None))
    out_specs = P(("row", "col"), None)
    return jax.shard_map(
        on_device, mesh=mesh, in_specs=in_specs, out_specs=out_specs, check_vma=False
    )
```

```python
import functools

import jax
import jax.numpy as jnp
from jax import lax
from jax.experimental import pallas as pl
from jax.experimental.pallas import tpu as pltpu
from jax.sharding import PartitionSpec as P

VMEM = pltpu.VMEM
SMEM = pltpu.SMEM
PIVOTS = 32
TERMS = ((0, 0), (0, 1), (1, 0), (1, 1), (0, 2), (2, 0))


def split(x, parts):
    out = []
    for i in range(parts):
        out.append(x.astype(jnp.bfloat16))
        if i < parts - 1:
            x = x - out[-1].astype(jnp.float32)
    return out


def dot_parts(a, b, contract):
    pairs = TERMS[: 3 if len(a) == 2 else 6]
    left = jnp.concatenate([a[i] for i, _ in pairs], axis=1)
    right = jnp.concatenate([b[j] for _, j in pairs], axis=contract)
    return lax.dot_general(
        left, right, (((1,), (contract,)), ((), ())), preferred_element_type=jnp.float32
    )


def by_terms(x, side):
    parts = split(x, 3)
    return jnp.concatenate([parts[term[side]] for term in TERMS], axis=0)


def one_pass(a, b):
    return jnp.dot(a, b, preferred_element_type=jnp.float32)


def spread(x, row):
    return jnp.broadcast_to(x[row : row + 1, :], (8, 128))


def sweep_panel(panel, base, lanes, subs):
    high = base >= 128
    q0 = base - jnp.where(high, 128, 0)
    low_half = [panel[8 * g : 8 * g + 8, :128] for g in range(4)]
    high_half = [panel[8 * g : 8 * g + 8, 128:] for g in range(4)]
    act = [jnp.where(high, h, l) for l, h in zip(low_half, high_half)]
    oth = [jnp.where(high, l, h) for l, h in zip(low_half, high_half)]

    def column(g, c):
        return jnp.take_along_axis(act[g], jnp.full((8, 128), q0 + c, jnp.int32), axis=1)

    diag = [column(0, l) for l in range(8)]
    for sb in range(4):
        cols = [[None] * 4 for _ in range(8)]
        later = [g for g in range(sb + 1, 4)] + [g for g in range(sb)]
        for g in later[:1]:
            for l in range(8):
                cols[l][g] = column(g, 8 * sb + l)
        following = [column(sb + 1, 8 * sb + 8 + l) for l in range(8)] if sb < 3 else None
        for g in later[1:]:
            for l in range(8):
                cols[l][g] = column(g, 8 * sb + l)
        invs, factors = [], [[None] * 8 for _ in range(8)]
        for l in range(8):
            at_row = subs == l
            inv = 1.0 / spread(diag[l], l)
            invs.append(inv)
            for m in range(l + 1, 8):
                t = spread(diag[m], l) * inv
                factors[l][m] = t
                diag[m] = jnp.where(at_row, t, diag[m] - diag[l] * t)
        for l in range(8):
            cols[l][sb] = diag[l]
        for g in later:
            for l in range(8):
                for m in range(l + 1, 8):
                    cols[m][g] = cols[m][g] - cols[l][g] * factors[l][m]
        if sb < 3:
            for l in range(8):
                scaled = cols[l][sb + 1] * invs[l]
                following = [f - cols[l][sb + 1] * spread(scaled, m) for m, f in enumerate(following)]
        for l in range(8):
            u = cols[l]
            at_row = subs == l
            at_lane = lanes == q0 + (8 * sb + l)
            inv = invs[l]
            row_act = jnp.where(at_lane, -inv, spread(act[sb], l) * inv)
            row_oth = spread(oth[sb], l) * inv
            act = [jnp.where(at_lane, 0.0, act[g]) - u[g] * row_act for g in range(4)]
            oth = [oth[g] - u[g] * row_oth for g in range(4)]
            act[sb] = jnp.where(at_row, row_act, act[sb])
            oth[sb] = jnp.where(at_row, row_oth, oth[sb])
        diag = following
    act, oth = jnp.concatenate(act, 0), jnp.concatenate(oth, 0)
    return jnp.concatenate(
        [jnp.where(high, oth, act), jnp.where(high, act, oth)], axis=1
    )


def invert_in_place(a_ref, panel_ref, swept_ref, trans_ref, beside):
    n = a_ref.shape[0]
    steps = n // PIVOTS
    lanes = lax.broadcasted_iota(jnp.int32, (8, 128), 1)
    subs = lax.broadcasted_iota(jnp.int32, (8, 128), 0)
    columns = lax.broadcasted_iota(jnp.int32, (n, n), 1)

    def inside(k, rows):
        return (columns[:rows] >= k * PIVOTS) & (columns[:rows] < (k + 1) * PIVOTS)

    def rows_of(k):
        return pl.ds(pl.multiple_of(k * PIVOTS, PIVOTS), PIVOTS)

    def apply(k, slot):
        a_ref[...] = jnp.where(inside(k, n), 0.0, a_ref[...]) - one_pass(
            trans_ref[slot], by_terms(swept_ref[slot], 1)
        )

    panel_ref[...] = a_ref[:PIVOTS, :]
    swept_ref[1] = jnp.zeros_like(panel_ref)
    trans_ref[1] = jnp.zeros(trans_ref.shape[1:], jnp.bfloat16)

    def step(k, carry):
        now, before = k % 2, (k + 1) % 2
        panel = panel_ref[...]
        trans_ref[now] = by_terms(panel, 0).T
        beside(k)
        swept = sweep_panel(panel, k * PIVOTS, lanes, subs)
        apply(k - 1, before)
        last = jnp.maximum(k - 1, 0)
        a_ref[rows_of(last), :] = jnp.where(k > 0, swept_ref[before], a_ref[rows_of(last), :])
        following = jnp.minimum(k + 1, steps - 1)
        panel_ref[...] = jnp.where(inside(k, PIVOTS), 0.0, a_ref[rows_of(following), :]) - one_pass(
            trans_ref[now, rows_of(following), :], by_terms(swept, 1)
        )
        swept_ref[now] = swept
        return carry

    lax.fori_loop(0, steps, step, 0)
    final = (steps - 1) % 2
    apply(steps - 1, final)
    a_ref[n - PIVOTS :, :] = swept_ref[final]


def pick_kernel(rows_ref, mask_ref, x_ref, out_ref, held):
    members = x_ref.shape[1]
    per_dev = held.shape[0] // 2
    start = lax.axis_index("col") * per_dev
    for b in range(2):
        for i in range(per_dev):
            r = rows_ref[b, start + i]
            held[b * per_dev + i : b * per_dev + i + 1, :] = x_ref[pl.ds(r, 1), :]
    chunks = members // 128
    lanes = lax.broadcasted_iota(jnp.int32, (1, 128), 1)
    kept = jnp.where(lanes == 0, mask_ref[0, 0, 0], mask_ref[0, 0, 1]).astype(jnp.float32)
    for piece in range(out_ref.shape[0]):
        g, j = piece // chunks, piece % chunks
        for s in range(8):
            out_ref[piece, :, 128 * s : 128 * s + 128] = held[8 * g + s : 8 * g + s + 1, 128 * j : 128 * j + 128]
        out_ref[piece, :, 1024:] = kept


def share_kernel(line_ref, out_ref, kept_ref, held):
    for c in range(line_ref.shape[0]):
        for s in range(8):
            held[c, s : s + 1, :] = line_ref[c, :, 128 * s : 128 * s + 128]
        kept_ref[c : c + 1, :] = line_ref[c, :, 1024:]
    for d in range(out_ref.shape[0]):
        out_ref[d] = held[...]


def prepare_kernel(
    owner_ref, mask_ref, x_ref, rows_ref, given_ref, var_ref,
    wanted_ref, rho_ref, decay_ref, anom_ref, mean_ref, value_ref, held_var_ref, *, nrows, ncols, local_len,
):
    rows_dev, members = x_ref.shape
    n = rows_ref.shape[1]
    per_dev = n // ncols
    place = lax.broadcasted_iota(jnp.int32, wanted_ref.shape, 1)
    early = lax.axis_index("row") < nrows // 2
    wanted_ref[...] = jnp.where((place < 1024) & early, owner_ref[0], owner_ref[1])
    lane = lax.broadcasted_iota(jnp.int32, (1, n), 1)
    first = (lax.axis_index("row") * ncols + lax.axis_index("col")) * rows_dev
    here = first + lax.broadcasted_iota(jnp.int32, (rows_dev, 1), 0)
    sub = lax.broadcasted_iota(jnp.int32, (n, 1), 0)
    diag = lax.broadcasted_iota(jnp.int32, (n, n), 0) == lax.broadcasted_iota(jnp.int32, (n, n), 1)

    def column(row):
        return jnp.sum(jnp.where(diag, row, 0.0), axis=1, keepdims=True)

    seen = column(rows_ref[1:2, :].astype(jnp.float32)).astype(jnp.int32)
    there = (owner_ref[1] * ncols + sub // per_dev) * rows_dev + seen

    def decay(positions, b):
        glob = (owner_ref[b] * ncols + lane // per_dev) * rows_dev + rows_ref[b : b + 1, :]
        dist = jnp.abs(positions - glob).astype(jnp.float32)
        return jnp.exp(-dist / jnp.float32(local_len))

    for b in range(2):
        mask = jnp.where(lane < 128, mask_ref[b, 0, 0], mask_ref[b, 0, 1]).astype(jnp.float32)
        rho_ref[b] = decay(here, b) * mask
    decay_ref[...] = decay(there, 0)
    x = x_ref[...]
    mean = jnp.sum(x, axis=1, keepdims=True) * (1.0 / members)
    anom_ref[...] = x - mean
    mean_ref[...] = jnp.broadcast_to(mean, mean_ref.shape)
    held = lax.broadcasted_iota(jnp.int32, value_ref.shape, 1)
    value_ref[...] = jnp.where(held == 0, column(given_ref[0:1, :]), column(given_ref[1:2, :]))
    held_var_ref[...] = var_ref[...]


def assimilate_kernel(
    own_ref, other_ref, kept_ref, rho_ref, decay_ref, x_ref, x_mean_ref, value_ref, var_ref,
    out_ref, q_ref, s0_ref, s1_ref, t_ref, c_ref, g_ref, mean_ref, panel_ref, swept_ref, trans_ref,
    v_ref, innov_ref, w_ref, v1_ref, e_ref, stage_ref, sems,
):
    rows_dev, members = x_ref.shape
    n = var_ref.shape[1]
    ncols = kept_ref.shape[0]
    per_dev = n // ncols
    groups = per_dev // 8
    chunks = members // 128
    core = lax.axis_index("row") & 1
    scale = 1.0 / (members - 1.0)
    obs1, obs0 = rows_dev, rows_dev + n

    def member_chunk(i, side):
        return pl.ds(pl.multiple_of((2 * i + (core if side == 0 else 1 - core)) * 128, 128), 128)

    def chunk(j, width):
        return pl.ds(pl.multiple_of(j * width, width), width)

    def observed(b, i, ref):
        return jnp.concatenate(
            [ref[(b * groups + g) * (chunks // 2) + i, c] for c in range(ncols) for g in range(groups)], axis=0
        )

    def add_up(c, carry):
        for b, top in ((0, obs0), (1, obs1)):
            for g in range(groups):
                slots = [(b * groups + g) * (chunks // 2) + i for i in range(chunks // 2)]
                total = own_ref[slots[0], c] + other_ref[slots[0], c]
                for slot in slots[1:]:
                    total = total + (own_ref[slot, c] + other_ref[slot, c])
                mean_ref[pl.ds(pl.multiple_of(top + c * per_dev + g * 8, 8), 8), :] = total
        return carry

    lax.fori_loop(0, ncols, add_up, 0)
    mean = jnp.sum(mean_ref[obs1:, :], axis=1, keepdims=True) * (1.0 / members)
    mean_ref[obs1:, :] = jnp.broadcast_to(mean, (2 * n, 128))
    mean_ref[:rows_dev, :] = x_mean_ref[...]

    wide = 2 * 128
    diag = lax.broadcasted_iota(jnp.int32, (n, n), 0) == lax.broadcasted_iota(jnp.int32, (n, n), 1)
    c_ref[...] = jnp.zeros_like(c_ref)

    def covariance0(i, carry):
        mean = mean_ref[obs0:, :]
        anom = jnp.concatenate([observed(0, i, own_ref) - mean, observed(0, i, other_ref) - mean], axis=1)
        parts = split(anom, 3)
        for p in range(3):
            s0_ref[p, :, chunk(i, wide)] = parts[p]
        c_ref[...] += dot_parts(parts, parts, 1)
        return carry

    lax.fori_loop(0, members // wide, covariance0, 0)
    for p, part in enumerate(split(c_ref[...], 3)):
        w_ref[p] = part
    c_ref[...] = c_ref[...] * scale + jnp.where(diag, var_ref[0:1, :], 0.0)
    t_ref[...] = jnp.zeros_like(t_ref)
    e_ref[...] = jnp.zeros_like(e_ref)

    def cross0(j):
        at, i, side = chunk(j, 128), j // 2, j % 2
        local = jnp.where(side == 0, x_ref[:, member_chunk(i, 0)], x_ref[:, member_chunk(i, 1)])
        seen = jnp.where(side == 0, observed(1, i, own_ref), observed(1, i, other_ref))
        for top, anom in ((0, local), (obs1, seen - mean_ref[obs1:obs0, :])):
            rows = slice(top, top + anom.shape[0])
            q_ref[rows, at] = anom
            parts = split(anom, 3)
            t_ref[rows, :] += dot_parts(parts, [s0_ref[p, :, at] for p in range(3)], 1)
            if top:
                e_ref[...] += dot_parts(parts, parts, 1)

    invert_in_place(c_ref, panel_ref, swept_ref, trans_ref, cross0)

    for p, part in enumerate(split(c_ref[...], 3)):
        v_ref[p] = part

    def gain(tapered, parts):
        return split(dot_parts(split(tapered, 3), [v_ref[p] for p in range(3)], 0), parts)

    for half in range(2):
        kept = jnp.concatenate(
            [
                jnp.concatenate(
                    [jnp.broadcast_to(kept_ref[c : c + 1, i : i + 1] * -scale, (per_dev, 128)) for i in range(2)],
                    axis=1,
                )
                for c in range(half * ncols // 2, (half + 1) * ncols // 2)
            ],
            axis=0,
        )
        rows = slice(half * n // 2, (half + 1) * n // 2)
        at = slice(obs1 + half * n // 2, obs1 + (half + 1) * n // 2)
        for p, part in enumerate(gain(t_ref[at, :] * (decay_ref[rows, :] * kept), 3)):
            g_ref[p, at, :] = part

    for half in range(2):
        at = slice(obs1 + half * n // 2, obs1 + (half + 1) * n // 2)
        product = dot_parts([g_ref[p, at, :] for p in range(3)], [w_ref[p] for p in range(3)], 0)
        for p, part in enumerate(split(0.25 * product - t_ref[at, :], 3)):
            v1_ref[p, half * n // 2 : (half + 1) * n // 2, :] = part
    for half in range(2):
        at = slice(obs1 + half * n // 2, obs1 + (half + 1) * n // 2)
        c_ref[half * n // 2 : (half + 1) * n // 2, :] = dot_parts(
            [g_ref[p, at, :] for p in range(3)], [v1_ref[p] for p in range(3)], 1
        )
    c_ref[...] = (e_ref[...] + 0.5 * (c_ref[...] + c_ref[...].T)) * scale + jnp.where(diag, var_ref[1:2, :], 0.0)

    for p, part in enumerate(gain(t_ref[:rows_dev, :] * (rho_ref[0] * -scale), 2)):
        g_ref[p, :rows_dev, :] = part
    for p, part in enumerate(split(value_ref[:, 0:1] - mean_ref[obs0:, :], 3)):
        innov_ref[p] = part
    t_ref[:rows_dev, :] = jnp.zeros((rows_dev, n), jnp.float32)

    def cross1(j):
        at = chunk(j, 128)
        some = pl.ds(pl.multiple_of(obs1 + j * (n // chunks), n // chunks), n // chunks)
        mean_ref[some, :] += dot_parts(
            [g_ref[p, some, :] for p in range(3)], [innov_ref[p] for p in range(3)], 0
        )
        some = chunk(j, rows_dev // chunks)
        mean_ref[some, :] += dot_parts(
            [g_ref[p, some, :] for p in range(2)], [innov_ref[p] for p in range(2)], 0
        )
        change = dot_parts(
            [g_ref[p, obs1:obs0, :] for p in range(3)], [s0_ref[p, :, at] for p in range(3)], 0
        )
        seen = split(q_ref[obs1:obs0, at] - 0.5 * change, 3)
        for p in range(3):
            s1_ref[p, :, at] = seen[p]
        change = dot_parts(
            [g_ref[p, :rows_dev, :] for p in range(2)], [s0_ref[p, :, at] for p in range(2)], 0
        )
        anom = q_ref[:rows_dev, at] - 0.5 * change
        q_ref[:rows_dev, at] = anom
        t_ref[:rows_dev, :] += dot_parts(split(anom, 3), seen, 1)

    invert_in_place(c_ref, panel_ref, swept_ref, trans_ref, cross1)
    innov1 = split(value_ref[:, 1:2] - mean_ref[obs1:obs0, :], 2)
    for p, part in enumerate(split(c_ref[...], 3)):
        v_ref[p] = part
    gain1 = gain(t_ref[:rows_dev, :] * (rho_ref[1] * -scale), 2)
    mean = mean_ref[:rows_dev, :] + dot_parts(gain1, innov1, 0)
    copies = []
    for i in range(members // wide):
        at = slice(i * wide, (i + 1) * wide)
        change = dot_parts(gain1, [s1_ref[p, :, at] for p in range(2)], 0)
        stage_ref[:, at] = jnp.concatenate([mean] * 2, axis=1) + q_ref[:rows_dev, at] - 0.5 * change
        for side in range(2):
            j = 2 * i + side
            copies.append(
                pltpu.make_async_copy(
                    stage_ref.at[:, 128 * j : 128 * j + 128], out_ref.at[:, member_chunk(i, side)], sems.at[j]
                )
            )
            copies[-1].start()
    for copy in copies:
        copy.wait()


def on_core(kernel, name, outs, smem, vmem, scratch=(), limit_mib=6):
    return pl.pallas_call(
        kernel,
        out_shape=outs,
        in_specs=[pl.BlockSpec(memory_space=SMEM)] * len(smem) + [pl.BlockSpec(memory_space=VMEM)] * len(vmem),
        out_specs=jax.tree.map(lambda _: pl.BlockSpec(memory_space=VMEM), outs),
        scratch_shapes=list(scratch),
        compiler_params=pltpu.CompilerParams(vmem_limit_bytes=limit_mib and limit_mib * 1024 * 1024),
        name=name,
    )(*smem, *vmem)


def exchange(x, axis, groups=None):
    return lax.all_to_all(x, axis, split_axis=0, concat_axis=0, axis_index_groups=groups, tiled=True)


def floats(*shape):
    return jax.ShapeDtypeStruct(shape, jnp.float32)


def prepare(owner, taper_mask, ensemble, obs_rows, obs_value, obs_var, nrows, ncols, local_len):
    rows_dev, members = ensemble.shape
    n = obs_rows.shape[1]
    return on_core(
        functools.partial(prepare_kernel, nrows=nrows, ncols=ncols, local_len=local_len), "prepare",
        (jax.ShapeDtypeStruct((1, 1024 + 128), jnp.int32), floats(2, rows_dev, n), floats(n, n), floats(rows_dev, members), floats(rows_dev, 128),
         floats(n, 128), floats(2, n)),
        (owner, taper_mask), (ensemble, obs_rows, obs_value, obs_var), limit_mib=None,
    )


def assimilate(own, other, kept, prepared):
    rows_dev, members = prepared[2].shape
    n = prepared[1].shape[0]
    total = rows_dev + 2 * n
    return pl.pallas_call(
        assimilate_kernel,
        out_shape=floats(rows_dev, members),
        in_specs=[pl.BlockSpec(memory_space=VMEM)] * (3 + len(prepared)),
        out_specs=pl.BlockSpec(memory_space=pl.ANY),
        scratch_shapes=[
            VMEM((rows_dev + n, members), jnp.float32),
            VMEM((3, n, members), jnp.bfloat16),
            VMEM((3, n, members), jnp.bfloat16),
            VMEM((rows_dev + n, n), jnp.float32),
            VMEM((n, n), jnp.float32),
            VMEM((3, rows_dev + n, n), jnp.bfloat16),
            VMEM((total, 128), jnp.float32),
            VMEM((PIVOTS, n), jnp.float32),
            VMEM((2, PIVOTS, n), jnp.float32),
            VMEM((2, n, len(TERMS) * PIVOTS), jnp.bfloat16),
            VMEM((3, n, n), jnp.bfloat16),
            VMEM((3, n, 128), jnp.bfloat16),
            VMEM((3, n, n), jnp.bfloat16),
            VMEM((3, n, n), jnp.bfloat16),
            VMEM((n, n), jnp.float32),
            VMEM((rows_dev, members), jnp.float32),
            pltpu.SemaphoreType.DMA((members // 128,)),
        ],
        compiler_params=pltpu.CompilerParams(vmem_limit_bytes=40 * 1024 * 1024),
        name="assimilate",
    )(own, other, kept, *prepared)


def on_device(ensemble, obs_rows, owner, obs_value, obs_var, taper_mask):
    rows, members = ensemble.shape
    ncols, nrows = lax.axis_size("col"), lax.axis_size("row")
    per_dev = obs_rows.shape[1] // ncols
    picked = on_core(
        pick_kernel, "pick_rows", floats(nrows, 1, 1024 + 128),
        (obs_rows, taper_mask), (ensemble,), [VMEM((2 * per_dev, members), jnp.float32)], None,
    )
    pieces = exchange(picked, "row")
    prepared = prepare(owner, taper_mask, ensemble, obs_rows, obs_value, obs_var, nrows, ncols, rows * nrows * ncols // 4)
    pieces, wanted, *prepared = lax.optimization_barrier((pieces, *prepared))
    taken = jnp.arange(nrows, dtype=jnp.int32)[:, None, None] == wanted[None]
    line = jnp.sum(jnp.where(taken, pieces, 0.0), axis=0)
    line = jnp.broadcast_to(line[None], (ncols, 1, 1024 + 128))
    line = exchange(line, "col")
    wide, kept = on_core(
        share_kernel, "share", (floats(nrows // 2, ncols, 8, 128), floats(ncols, 128)),
        (), (line,), [VMEM((ncols, 8, 128), jnp.float32)],
    )
    own = exchange(wide, "row", [[r for r in range(nrows) if r % 2 == c] for c in range(2)])
    other = lax.ppermute(own, "row", [(r, r ^ 1) for r in range(nrows)])
    return assimilate(own, other, kept, prepared)


def solution(mesh):
    in_specs = (P(("row", "col"), None), P(), P(), P(), P(), P(None, ("row", "col"), None))
    out_specs = P(("row", "col"), None)
    return jax.shard_map(
        on_device, mesh=mesh, in_specs=in_specs, out_specs=out_specs, check_vma=False
    )
```

```python
import functools

import jax
import jax.numpy as jnp
from jax import lax
from jax.experimental import pallas as pl
from jax.experimental.pallas import tpu as pltpu
from jax.sharding import PartitionSpec as P

VMEM = pltpu.VMEM
SMEM = pltpu.SMEM
PIVOTS = 32
TERMS = ((0, 0), (0, 1), (1, 0), (1, 1), (0, 2), (2, 0))


def split(x, parts):
    out = []
    for i in range(parts):
        out.append(x.astype(jnp.bfloat16))
        if i < parts - 1:
            x = x - out[-1].astype(jnp.float32)
    return out


def dot_parts(a, b, contract):
    pairs = TERMS[: 3 if len(a) == 2 else 6]
    left = jnp.concatenate([a[i] for i, _ in pairs], axis=1)
    right = jnp.concatenate([b[j] for _, j in pairs], axis=contract)
    return lax.dot_general(
        left, right, (((1,), (contract,)), ((), ())), preferred_element_type=jnp.float32
    )


def by_terms(x, side):
    parts = split(x, 3)
    return jnp.concatenate([parts[term[side]] for term in TERMS], axis=0)


def one_pass(a, b):
    return jnp.dot(a, b, preferred_element_type=jnp.float32)


def spread(x, row):
    return jnp.broadcast_to(x[row : row + 1, :], (8, 128))


def sweep_panel(panel, base, lanes, subs):
    high = base >= 128
    q0 = base - jnp.where(high, 128, 0)
    low_half = [panel[8 * g : 8 * g + 8, :128] for g in range(4)]
    high_half = [panel[8 * g : 8 * g + 8, 128:] for g in range(4)]
    act = [jnp.where(high, h, l) for l, h in zip(low_half, high_half)]
    oth = [jnp.where(high, l, h) for l, h in zip(low_half, high_half)]

    def column(g, c):
        return jnp.take_along_axis(act[g], jnp.full((8, 128), q0 + c, jnp.int32), axis=1)

    diag = [column(0, l) for l in range(8)]
    for sb in range(4):
        cols = [[None] * 4 for _ in range(8)]
        later = [g for g in range(sb + 1, 4)] + [g for g in range(sb)]
        for g in later[:1]:
            for l in range(8):
                cols[l][g] = column(g, 8 * sb + l)
        following = [column(sb + 1, 8 * sb + 8 + l) for l in range(8)] if sb < 3 else None
        for g in later[1:]:
            for l in range(8):
                cols[l][g] = column(g, 8 * sb + l)
        invs, factors = [], [[None] * 8 for _ in range(8)]
        for l in range(8):
            at_row = subs == l
            inv = 1.0 / spread(diag[l], l)
            invs.append(inv)
            for m in range(l + 1, 8):
                t = spread(diag[m], l) * inv
                factors[l][m] = t
                diag[m] = jnp.where(at_row, t, diag[m] - diag[l] * t)
        for l in range(8):
            cols[l][sb] = diag[l]
        for g in later:
            for l in range(8):
                for m in range(l + 1, 8):
                    cols[m][g] = cols[m][g] - cols[l][g] * factors[l][m]
        if sb < 3:
            for l in range(8):
                scaled = cols[l][sb + 1] * invs[l]
                following = [f - cols[l][sb + 1] * spread(scaled, m) for m, f in enumerate(following)]
        for l in range(8):
            u = cols[l]
            at_row = subs == l
            at_lane = lanes == q0 + (8 * sb + l)
            inv = invs[l]
            row_act = jnp.where(at_lane, -inv, spread(act[sb], l) * inv)
            row_oth = spread(oth[sb], l) * inv
            act = [jnp.where(at_lane, 0.0, act[g]) - u[g] * row_act for g in range(4)]
            oth = [oth[g] - u[g] * row_oth for g in range(4)]
            act[sb] = jnp.where(at_row, row_act, act[sb])
            oth[sb] = jnp.where(at_row, row_oth, oth[sb])
        diag = following
    act, oth = jnp.concatenate(act, 0), jnp.concatenate(oth, 0)
    return jnp.concatenate(
        [jnp.where(high, oth, act), jnp.where(high, act, oth)], axis=1
    )


def invert_in_place(a_ref, panel_ref, swept_ref, trans_ref, beside):
    n = a_ref.shape[0]
    steps = n // PIVOTS
    lanes = lax.broadcasted_iota(jnp.int32, (8, 128), 1)
    subs = lax.broadcasted_iota(jnp.int32, (8, 128), 0)
    columns = lax.broadcasted_iota(jnp.int32, (n, n), 1)

    def inside(k, rows):
        return (columns[:rows] >= k * PIVOTS) & (columns[:rows] < (k + 1) * PIVOTS)

    def rows_of(k):
        return pl.ds(pl.multiple_of(k * PIVOTS, PIVOTS), PIVOTS)

    def apply(k, slot):
        a_ref[...] = jnp.where(inside(k, n), 0.0, a_ref[...]) - one_pass(
            trans_ref[slot], by_terms(swept_ref[slot], 1)
        )

    panel_ref[...] = a_ref[:PIVOTS, :]
    swept_ref[1] = jnp.zeros_like(panel_ref)
    trans_ref[1] = jnp.zeros(trans_ref.shape[1:], jnp.bfloat16)

    def step(k, carry):
        now, before = k % 2, (k + 1) % 2
        panel = panel_ref[...]
        trans_ref[now] = by_terms(panel, 0).T
        beside(k)
        swept = sweep_panel(panel, k * PIVOTS, lanes, subs)
        apply(k - 1, before)
        last = jnp.maximum(k - 1, 0)
        a_ref[rows_of(last), :] = jnp.where(k > 0, swept_ref[before], a_ref[rows_of(last), :])
        following = jnp.minimum(k + 1, steps - 1)
        panel_ref[...] = jnp.where(inside(k, PIVOTS), 0.0, a_ref[rows_of(following), :]) - one_pass(
            trans_ref[now, rows_of(following), :], by_terms(swept, 1)
        )
        swept_ref[now] = swept
        return carry

    lax.fori_loop(0, steps, step, 0)
    final = (steps - 1) % 2
    apply(steps - 1, final)
    a_ref[n - PIVOTS :, :] = swept_ref[final]


def pick_kernel(rows_ref, mask_ref, x_ref, out_ref, held):
    members = x_ref.shape[1]
    per_dev = held.shape[0] // 2
    start = lax.axis_index("col") * per_dev
    for b in range(2):
        for i in range(per_dev):
            r = rows_ref[b, start + i]
            held[b * per_dev + i : b * per_dev + i + 1, :] = x_ref[pl.ds(r, 1), :]
    chunks = members // 128
    lanes = lax.broadcasted_iota(jnp.int32, (1, 128), 1)
    kept = jnp.where(lanes == 0, mask_ref[0, 0, 0], mask_ref[0, 0, 1]).astype(jnp.float32)
    for piece in range(out_ref.shape[0]):
        g, j = piece // chunks, piece % chunks
        for s in range(8):
            out_ref[piece, :, 128 * s : 128 * s + 128] = held[8 * g + s : 8 * g + s + 1, 128 * j : 128 * j + 128]
        out_ref[piece, :, 1024:] = kept


def choose_kernel(owner_ref, wanted_ref, *, nrows):
    place = lax.broadcasted_iota(jnp.int32, wanted_ref.shape, 1)
    early = lax.axis_index("row") < nrows // 2
    wanted_ref[...] = jnp.where((place < 1024) & early, owner_ref[0], owner_ref[1])


def share_kernel(line_ref, out_ref, kept_ref, held):
    for c in range(line_ref.shape[0]):
        for s in range(8):
            held[c, s : s + 1, :] = line_ref[c, :, 128 * s : 128 * s + 128]
        kept_ref[c : c + 1, :] = line_ref[c, :, 1024:]
    for d in range(out_ref.shape[0]):
        out_ref[d] = held[...]


def prepare_kernel(
    owner_ref, mask_ref, x_ref, rows_ref, given_ref, var_ref,
    rho_ref, decay_ref, anom_ref, mean_ref, value_ref, held_var_ref, *, ncols, local_len,
):
    rows_dev, members = x_ref.shape
    n = rows_ref.shape[1]
    per_dev = n // ncols
    lane = lax.broadcasted_iota(jnp.int32, (1, n), 1)
    first = (lax.axis_index("row") * ncols + lax.axis_index("col")) * rows_dev
    here = first + lax.broadcasted_iota(jnp.int32, (rows_dev, 1), 0)
    sub = lax.broadcasted_iota(jnp.int32, (n, 1), 0)
    diag = lax.broadcasted_iota(jnp.int32, (n, n), 0) == lax.broadcasted_iota(jnp.int32, (n, n), 1)

    def column(row):
        return jnp.sum(jnp.where(diag, row, 0.0), axis=1, keepdims=True)

    seen = column(rows_ref[1:2, :].astype(jnp.float32)).astype(jnp.int32)
    there = (owner_ref[1] * ncols + sub // per_dev) * rows_dev + seen

    def decay(positions, b):
        glob = (owner_ref[b] * ncols + lane // per_dev) * rows_dev + rows_ref[b : b + 1, :]
        dist = jnp.abs(positions - glob).astype(jnp.float32)
        return jnp.exp(-dist / jnp.float32(local_len))

    for b in range(2):
        mask = jnp.where(lane < 128, mask_ref[b, 0, 0], mask_ref[b, 0, 1]).astype(jnp.float32)
        rho_ref[b] = decay(here, b) * mask
    decay_ref[...] = decay(there, 0)
    x = x_ref[...]
    mean = jnp.sum(x, axis=1, keepdims=True) * (1.0 / members)
    anom_ref[...] = x - mean
    mean_ref[...] = jnp.broadcast_to(mean, mean_ref.shape)
    held = lax.broadcasted_iota(jnp.int32, value_ref.shape, 1)
    value_ref[...] = jnp.where(held == 0, column(given_ref[0:1, :]), column(given_ref[1:2, :]))
    held_var_ref[...] = var_ref[...]


def assimilate_kernel(
    own_ref, other_ref, kept_ref, rho_ref, decay_ref, x_ref, x_mean_ref, value_ref, var_ref,
    out_ref, q_ref, s0_ref, s1_ref, t_ref, c_ref, g_ref, mean_ref, panel_ref, swept_ref, trans_ref,
    v_ref, innov_ref, w_ref, v1_ref, e_ref, stage_ref, sems,
):
    rows_dev, members = x_ref.shape
    n = var_ref.shape[1]
    ncols = kept_ref.shape[0]
    per_dev = n // ncols
    groups = per_dev // 8
    chunks = members // 128
    core = lax.axis_index("row") & 1
    scale = 1.0 / (members - 1.0)
    obs1, obs0 = rows_dev, rows_dev + n

    def member_chunk(i, side):
        return pl.ds(pl.multiple_of((2 * i + (core if side == 0 else 1 - core)) * 128, 128), 128)

    def chunk(j, width):
        return pl.ds(pl.multiple_of(j * width, width), width)

    def observed(b, i, ref):
        return jnp.concatenate(
            [ref[(b * groups + g) * (chunks // 2) + i, c] for c in range(ncols) for g in range(groups)], axis=0
        )

    def add_up(c, carry):
        for b, top in ((0, obs0), (1, obs1)):
            for g in range(groups):
                slots = [(b * groups + g) * (chunks // 2) + i for i in range(chunks // 2)]
                total = own_ref[slots[0], c] + other_ref[slots[0], c]
                for slot in slots[1:]:
                    total = total + (own_ref[slot, c] + other_ref[slot, c])
                mean_ref[pl.ds(pl.multiple_of(top + c * per_dev + g * 8, 8), 8), :] = total
        return carry

    lax.fori_loop(0, ncols, add_up, 0, unroll=4)
    mean = jnp.sum(mean_ref[obs1:, :], axis=1, keepdims=True) * (1.0 / members)
    mean_ref[obs1:, :] = jnp.broadcast_to(mean, (2 * n, 128))
    mean_ref[:rows_dev, :] = x_mean_ref[...]

    wide = 2 * 128
    diag = lax.broadcasted_iota(jnp.int32, (n, n), 0) == lax.broadcasted_iota(jnp.int32, (n, n), 1)
    c_ref[...] = jnp.zeros_like(c_ref)

    def covariance0(i, carry):
        mean = mean_ref[obs0:, :]
        anom = jnp.concatenate([observed(0, i, own_ref) - mean, observed(0, i, other_ref) - mean], axis=1)
        parts = split(anom, 3)
        for p in range(3):
            s0_ref[p, :, chunk(i, wide)] = parts[p]
        c_ref[...] += dot_parts(parts, parts, 1)
        return carry

    lax.fori_loop(0, members // wide, covariance0, 0, unroll=4)
    for p, part in enumerate(split(c_ref[...], 3)):
        w_ref[p] = part
    c_ref[...] = c_ref[...] * scale + jnp.where(diag, var_ref[0:1, :], 0.0)
    t_ref[...] = jnp.zeros_like(t_ref)
    e_ref[...] = jnp.zeros_like(e_ref)

    def cross0(j):
        at, i, side = chunk(j, 128), j // 2, j % 2
        local = jnp.where(side == 0, x_ref[:, member_chunk(i, 0)], x_ref[:, member_chunk(i, 1)])
        seen = jnp.where(side == 0, observed(1, i, own_ref), observed(1, i, other_ref))
        for top, anom in ((0, local), (obs1, seen - mean_ref[obs1:obs0, :])):
            rows = slice(top, top + anom.shape[0])
            q_ref[rows, at] = anom
            parts = split(anom, 3)
            t_ref[rows, :] += dot_parts(parts, [s0_ref[p, :, at] for p in range(3)], 1)
            if top:
                e_ref[...] += dot_parts(parts, parts, 1)

    invert_in_place(c_ref, panel_ref, swept_ref, trans_ref, cross0)

    for p, part in enumerate(split(c_ref[...], 3)):
        v_ref[p] = part

    def gain(tapered, parts):
        return split(dot_parts(split(tapered, 3), [v_ref[p] for p in range(3)], 0), parts)

    for half in range(2):
        kept = jnp.concatenate(
            [
                jnp.concatenate(
                    [jnp.broadcast_to(kept_ref[c : c + 1, i : i + 1] * -scale, (per_dev, 128)) for i in range(2)],
                    axis=1,
                )
                for c in range(half * ncols // 2, (half + 1) * ncols // 2)
            ],
            axis=0,
        )
        rows = slice(half * n // 2, (half + 1) * n // 2)
        at = slice(obs1 + half * n // 2, obs1 + (half + 1) * n // 2)
        for p, part in enumerate(gain(t_ref[at, :] * (decay_ref[rows, :] * kept), 3)):
            g_ref[p, at, :] = part

    for half in range(2):
        at = slice(obs1 + half * n // 2, obs1 + (half + 1) * n // 2)
        product = dot_parts([g_ref[p, at, :] for p in range(3)], [w_ref[p] for p in range(3)], 0)
        for p, part in enumerate(split(0.25 * product - t_ref[at, :], 3)):
            v1_ref[p, half * n // 2 : (half + 1) * n // 2, :] = part
    for half in range(2):
        at = slice(obs1 + half * n // 2, obs1 + (half + 1) * n // 2)
        c_ref[half * n // 2 : (half + 1) * n // 2, :] = dot_parts(
            [g_ref[p, at, :] for p in range(3)], [v1_ref[p] for p in range(3)], 1
        )
    c_ref[...] = (e_ref[...] + 0.5 * (c_ref[...] + c_ref[...].T)) * scale + jnp.where(diag, var_ref[1:2, :], 0.0)

    for p, part in enumerate(gain(t_ref[:rows_dev, :] * (rho_ref[0] * -scale), 2)):
        g_ref[p, :rows_dev, :] = part
    for p, part in enumerate(split(value_ref[:, 0:1] - mean_ref[obs0:, :], 3)):
        innov_ref[p] = part
    t_ref[:rows_dev, :] = jnp.zeros((rows_dev, n), jnp.float32)

    def cross1(j):
        at = chunk(j, 128)
        some = pl.ds(pl.multiple_of(obs1 + j * (n // chunks), n // chunks), n // chunks)
        mean_ref[some, :] += dot_parts(
            [g_ref[p, some, :] for p in range(3)], [innov_ref[p] for p in range(3)], 0
        )
        some = chunk(j, rows_dev // chunks)
        mean_ref[some, :] += dot_parts(
            [g_ref[p, some, :] for p in range(2)], [innov_ref[p] for p in range(2)], 0
        )
        change = dot_parts(
            [g_ref[p, obs1:obs0, :] for p in range(3)], [s0_ref[p, :, at] for p in range(3)], 0
        )
        seen = split(q_ref[obs1:obs0, at] - 0.5 * change, 3)
        for p in range(3):
            s1_ref[p, :, at] = seen[p]
        change = dot_parts(
            [g_ref[p, :rows_dev, :] for p in range(2)], [s0_ref[p, :, at] for p in range(2)], 0
        )
        anom = q_ref[:rows_dev, at] - 0.5 * change
        q_ref[:rows_dev, at] = anom
        t_ref[:rows_dev, :] += dot_parts(split(anom, 3), seen, 1)

    invert_in_place(c_ref, panel_ref, swept_ref, trans_ref, cross1)
    innov1 = split(value_ref[:, 1:2] - mean_ref[obs1:obs0, :], 2)
    for p, part in enumerate(split(c_ref[...], 3)):
        v_ref[p] = part
    gain1 = gain(t_ref[:rows_dev, :] * (rho_ref[1] * -scale), 2)
    mean = mean_ref[:rows_dev, :] + dot_parts(gain1, innov1, 0)
    copies = []
    for i in range(members // wide):
        at = slice(i * wide, (i + 1) * wide)
        change = dot_parts(gain1, [s1_ref[p, :, at] for p in range(2)], 0)
        stage_ref[:, at] = jnp.concatenate([mean] * 2, axis=1) + q_ref[:rows_dev, at] - 0.5 * change
        for side in range(2):
            j = 2 * i + side
            copies.append(
                pltpu.make_async_copy(
                    stage_ref.at[:, 128 * j : 128 * j + 128], out_ref.at[:, member_chunk(i, side)], sems.at[j]
                )
            )
            copies[-1].start()
    for copy in copies:
        copy.wait()


def on_core(kernel, name, outs, smem, vmem, scratch=(), limit_mib=6):
    return pl.pallas_call(
        kernel,
        out_shape=outs,
        in_specs=[pl.BlockSpec(memory_space=SMEM)] * len(smem) + [pl.BlockSpec(memory_space=VMEM)] * len(vmem),
        out_specs=jax.tree.map(lambda _: pl.BlockSpec(memory_space=VMEM), outs),
        scratch_shapes=list(scratch),
        compiler_params=pltpu.CompilerParams(vmem_limit_bytes=limit_mib and limit_mib * 1024 * 1024),
        name=name,
    )(*smem, *vmem)


def exchange(x, axis, groups=None):
    return lax.all_to_all(x, axis, split_axis=0, concat_axis=0, axis_index_groups=groups, tiled=True)


def floats(*shape):
    return jax.ShapeDtypeStruct(shape, jnp.float32)


def prepare(owner, taper_mask, ensemble, obs_rows, obs_value, obs_var, ncols, local_len):
    rows_dev, members = ensemble.shape
    n = obs_rows.shape[1]
    return on_core(
        functools.partial(prepare_kernel, ncols=ncols, local_len=local_len), "prepare",
        (floats(2, rows_dev, n), floats(n, n), floats(rows_dev, members), floats(rows_dev, 128),
         floats(n, 128), floats(2, n)),
        (owner, taper_mask), (ensemble, obs_rows, obs_value, obs_var), limit_mib=None,
    )


def assimilate(own, other, kept, prepared):
    rows_dev, members = prepared[2].shape
    n = prepared[1].shape[0]
    total = rows_dev + 2 * n
    return pl.pallas_call(
        assimilate_kernel,
        out_shape=floats(rows_dev, members),
        in_specs=[pl.BlockSpec(memory_space=VMEM)] * (3 + len(prepared)),
        out_specs=pl.BlockSpec(memory_space=pl.ANY),
        scratch_shapes=[
            VMEM((rows_dev + n, members), jnp.float32),
            VMEM((3, n, members), jnp.bfloat16),
            VMEM((3, n, members), jnp.bfloat16),
            VMEM((rows_dev + n, n), jnp.float32),
            VMEM((n, n), jnp.float32),
            VMEM((3, rows_dev + n, n), jnp.bfloat16),
            VMEM((total, 128), jnp.float32),
            VMEM((PIVOTS, n), jnp.float32),
            VMEM((2, PIVOTS, n), jnp.float32),
            VMEM((2, n, len(TERMS) * PIVOTS), jnp.bfloat16),
            VMEM((3, n, n), jnp.bfloat16),
            VMEM((3, n, 128), jnp.bfloat16),
            VMEM((3, n, n), jnp.bfloat16),
            VMEM((3, n, n), jnp.bfloat16),
            VMEM((n, n), jnp.float32),
            VMEM((rows_dev, members), jnp.float32),
            pltpu.SemaphoreType.DMA((members // 128,)),
        ],
        compiler_params=pltpu.CompilerParams(vmem_limit_bytes=40 * 1024 * 1024),
        name="assimilate",
    )(own, other, kept, *prepared)


def on_device(ensemble, obs_rows, owner, obs_value, obs_var, taper_mask):
    rows, members = ensemble.shape
    ncols, nrows = lax.axis_size("col"), lax.axis_size("row")
    per_dev = obs_rows.shape[1] // ncols
    picked = on_core(
        pick_kernel, "pick_rows", floats(nrows, 1, 1024 + 128),
        (obs_rows, taper_mask), (ensemble,), [VMEM((2 * per_dev, members), jnp.float32)], None,
    )
    pieces = exchange(picked, "row")
    prepared = prepare(owner, taper_mask, ensemble, obs_rows, obs_value, obs_var, ncols, rows * nrows * ncols // 4)
    wanted = on_core(
        functools.partial(choose_kernel, nrows=nrows), "choose",
        jax.ShapeDtypeStruct((1, 1024 + 128), jnp.int32), (owner,), (),
    )
    pieces, wanted, *prepared = lax.optimization_barrier((pieces, wanted, *prepared))
    taken = jnp.arange(nrows, dtype=jnp.int32)[:, None, None] == wanted[None]
    line = jnp.sum(jnp.where(taken, pieces, 0.0), axis=0)
    line = jnp.broadcast_to(line[None], (ncols, 1, 1024 + 128))
    line = exchange(line, "col")
    wide, kept = on_core(
        share_kernel, "share", (floats(nrows // 2, ncols, 8, 128), floats(ncols, 128)),
        (), (line,), [VMEM((ncols, 8, 128), jnp.float32)],
    )
    own = exchange(wide, "row", [[r for r in range(nrows) if r % 2 == c] for c in range(2)])
    other = lax.ppermute(own, "row", [(r, r ^ 1) for r in range(nrows)])
    return assimilate(own, other, kept, prepared)


def solution(mesh):
    in_specs = (P(("row", "col"), None), P(), P(), P(), P(), P(None, ("row", "col"), None))
    out_specs = P(("row", "col"), None)
    return jax.shard_map(
        on_device, mesh=mesh, in_specs=in_specs, out_specs=out_specs, check_vma=False
    )
```

```python
import functools

import jax
import jax.numpy as jnp
from jax import lax
from jax.experimental import pallas as pl
from jax.experimental.pallas import tpu as pltpu
from jax.sharding import PartitionSpec as P

VMEM = pltpu.VMEM
SMEM = pltpu.SMEM
PIVOTS = 32
TERMS = ((0, 0), (0, 1), (1, 0), (1, 1), (0, 2), (2, 0))


def split(x, parts):
    out = []
    for i in range(parts):
        out.append(x.astype(jnp.bfloat16))
        if i < parts - 1:
            x = x - out[-1].astype(jnp.float32)
    return out


def dot_parts(a, b, contract):
    pairs = TERMS[: 3 if len(a) == 2 else 6]
    left = jnp.concatenate([a[i] for i, _ in pairs], axis=1)
    right = jnp.concatenate([b[j] for _, j in pairs], axis=contract)
    return lax.dot_general(
        left, right, (((1,), (contract,)), ((), ())), preferred_element_type=jnp.float32
    )


def by_terms(x, side):
    parts = split(x, 3)
    return jnp.concatenate([parts[term[side]] for term in TERMS], axis=0)


def one_pass(a, b):
    return jnp.dot(a, b, preferred_element_type=jnp.float32)


def spread(x, row):
    return jnp.broadcast_to(x[row : row + 1, :], (8, 128))


def sweep_panel(panel, base, lanes, subs):
    high = base >= 128
    q0 = base - jnp.where(high, 128, 0)
    low_half = [panel[8 * g : 8 * g + 8, :128] for g in range(4)]
    high_half = [panel[8 * g : 8 * g + 8, 128:] for g in range(4)]
    act = [jnp.where(high, h, l) for l, h in zip(low_half, high_half)]
    oth = [jnp.where(high, l, h) for l, h in zip(low_half, high_half)]

    def column(g, c):
        return jnp.take_along_axis(act[g], jnp.full((8, 128), q0 + c, jnp.int32), axis=1)

    diag = [column(0, l) for l in range(8)]
    for sb in range(4):
        cols = [[None] * 4 for _ in range(8)]
        later = [g for g in range(sb + 1, 4)] + [g for g in range(sb)]
        for g in later[:1]:
            for l in range(8):
                cols[l][g] = column(g, 8 * sb + l)
        following = [column(sb + 1, 8 * sb + 8 + l) for l in range(8)] if sb < 3 else None
        for g in later[1:]:
            for l in range(8):
                cols[l][g] = column(g, 8 * sb + l)
        invs, factors = [], [[None] * 8 for _ in range(8)]
        for l in range(8):
            at_row = subs == l
            inv = 1.0 / spread(diag[l], l)
            invs.append(inv)
            for m in range(l + 1, 8):
                t = spread(diag[m], l) * inv
                factors[l][m] = t
                diag[m] = jnp.where(at_row, t, diag[m] - diag[l] * t)
        for l in range(8):
            cols[l][sb] = diag[l]
        for g in later:
            for l in range(8):
                for m in range(l + 1, 8):
                    cols[m][g] = cols[m][g] - cols[l][g] * factors[l][m]
        if sb < 3:
            for l in range(8):
                scaled = cols[l][sb + 1] * invs[l]
                following = [f - cols[l][sb + 1] * spread(scaled, m) for m, f in enumerate(following)]
        for l in range(8):
            u = cols[l]
            at_row = subs == l
            at_lane = lanes == q0 + (8 * sb + l)
            inv = invs[l]
            row_act = jnp.where(at_lane, -inv, spread(act[sb], l) * inv)
            row_oth = spread(oth[sb], l) * inv
            act = [jnp.where(at_lane, 0.0, act[g]) - u[g] * row_act for g in range(4)]
            oth = [oth[g] - u[g] * row_oth for g in range(4)]
            act[sb] = jnp.where(at_row, row_act, act[sb])
            oth[sb] = jnp.where(at_row, row_oth, oth[sb])
        diag = following
    act, oth = jnp.concatenate(act, 0), jnp.concatenate(oth, 0)
    return jnp.concatenate(
        [jnp.where(high, oth, act), jnp.where(high, act, oth)], axis=1
    )


def invert_in_place(a_ref, panel_ref, swept_ref, trans_ref, beside):
    n = a_ref.shape[0]
    steps = n // PIVOTS
    lanes = lax.broadcasted_iota(jnp.int32, (8, 128), 1)
    subs = lax.broadcasted_iota(jnp.int32, (8, 128), 0)
    columns = lax.broadcasted_iota(jnp.int32, (n, n), 1)

    def inside(k, rows):
        return (columns[:rows] >= k * PIVOTS) & (columns[:rows] < (k + 1) * PIVOTS)

    def rows_of(k):
        return pl.ds(pl.multiple_of(k * PIVOTS, PIVOTS), PIVOTS)

    def apply(k, slot):
        a_ref[...] = jnp.where(inside(k, n), 0.0, a_ref[...]) - one_pass(
            trans_ref[slot], by_terms(swept_ref[slot], 1)
        )

    panel_ref[...] = a_ref[:PIVOTS, :]
    swept_ref[1] = jnp.zeros_like(panel_ref)
    trans_ref[1] = jnp.zeros(trans_ref.shape[1:], jnp.bfloat16)

    def step(k, carry):
        now, before = k % 2, (k + 1) % 2
        panel = panel_ref[...]
        trans_ref[now] = by_terms(panel, 0).T
        beside(k)
        swept = sweep_panel(panel, k * PIVOTS, lanes, subs)
        apply(k - 1, before)
        last = jnp.maximum(k - 1, 0)
        a_ref[rows_of(last), :] = jnp.where(k > 0, swept_ref[before], a_ref[rows_of(last), :])
        following = jnp.minimum(k + 1, steps - 1)
        panel_ref[...] = jnp.where(inside(k, PIVOTS), 0.0, a_ref[rows_of(following), :]) - one_pass(
            trans_ref[now, rows_of(following), :], by_terms(swept, 1)
        )
        swept_ref[now] = swept
        return carry

    lax.fori_loop(0, steps, step, 0)
    final = (steps - 1) % 2
    apply(steps - 1, final)
    a_ref[n - PIVOTS :, :] = swept_ref[final]


def pick_kernel(rows_ref, mask_ref, x_ref, out_ref, held):
    members = x_ref.shape[1]
    per_dev = held.shape[0] // 2
    start = lax.axis_index("col") * per_dev
    for b in range(2):
        for i in range(per_dev):
            r = rows_ref[b, start + i]
            held[b * per_dev + i : b * per_dev + i + 1, :] = x_ref[pl.ds(r, 1), :]
    chunks = members // 128
    lanes = lax.broadcasted_iota(jnp.int32, (1, 128), 1)
    kept = jnp.where(lanes == 0, mask_ref[0, 0, 0], mask_ref[0, 0, 1]).astype(jnp.float32)
    for piece in range(out_ref.shape[0]):
        g, j = piece // chunks, piece % chunks
        for s in range(8):
            out_ref[piece, :, 128 * s : 128 * s + 128] = held[8 * g + s : 8 * g + s + 1, 128 * j : 128 * j + 128]
        out_ref[piece, :, 1024:] = kept


def choose_kernel(owner_ref, wanted_ref, *, nrows):
    place = lax.broadcasted_iota(jnp.int32, wanted_ref.shape, 1)
    early = lax.axis_index("row") < nrows // 2
    wanted_ref[...] = jnp.where((place < 1024) & early, owner_ref[0], owner_ref[1])


def share_kernel(line_ref, out_ref, kept_ref, held):
    for c in range(line_ref.shape[0]):
        for s in range(8):
            held[c, s : s + 1, :] = line_ref[c, :, 128 * s : 128 * s + 128]
        kept_ref[c : c + 1, :] = line_ref[c, :, 1024:]
    for d in range(out_ref.shape[0]):
        out_ref[d] = held[...]


def prepare_kernel(
    owner_ref, mask_ref, x_ref, rows_ref, given_ref, var_ref,
    rho_ref, decay_ref, anom_ref, mean_ref, value_ref, held_var_ref, *, ncols, local_len,
):
    rows_dev, members = x_ref.shape
    n = rows_ref.shape[1]
    per_dev = n // ncols
    lane = lax.broadcasted_iota(jnp.int32, (1, n), 1)
    first = (lax.axis_index("row") * ncols + lax.axis_index("col")) * rows_dev
    here = first + lax.broadcasted_iota(jnp.int32, (rows_dev, 1), 0)
    sub = lax.broadcasted_iota(jnp.int32, (n, 1), 0)
    diag = lax.broadcasted_iota(jnp.int32, (n, n), 0) == lax.broadcasted_iota(jnp.int32, (n, n), 1)

    def column(row):
        return jnp.sum(jnp.where(diag, row, 0.0), axis=1, keepdims=True)

    seen = column(rows_ref[1:2, :].astype(jnp.float32)).astype(jnp.int32)
    there = (owner_ref[1] * ncols + sub // per_dev) * rows_dev + seen

    def decay(positions, b):
        glob = (owner_ref[b] * ncols + lane // per_dev) * rows_dev + rows_ref[b : b + 1, :]
        dist = jnp.abs(positions - glob).astype(jnp.float32)
        return jnp.exp(-dist / jnp.float32(local_len))

    for b in range(2):
        mask = jnp.where(lane < 128, mask_ref[b, 0, 0], mask_ref[b, 0, 1]).astype(jnp.float32)
        rho_ref[b] = decay(here, b) * mask
    decay_ref[...] = decay(there, 0)
    x = x_ref[...]
    mean = jnp.sum(x, axis=1, keepdims=True) * (1.0 / members)
    anom_ref[...] = x - mean
    mean_ref[...] = jnp.broadcast_to(mean, mean_ref.shape)
    held = lax.broadcasted_iota(jnp.int32, value_ref.shape, 1)
    value_ref[...] = jnp.where(held == 0, column(given_ref[0:1, :]), column(given_ref[1:2, :]))
    held_var_ref[...] = var_ref[...]


def assimilate_kernel(
    own_ref, other_ref, kept_ref, rho_ref, decay_ref, x_ref, x_mean_ref, value_ref, var_ref,
    out_ref, q_ref, s0_ref, s1_ref, t_ref, c_ref, g_ref, mean_ref, panel_ref, swept_ref, trans_ref,
    v_ref, innov_ref, w_ref, v1_ref, e_ref, stage_ref, sems,
):
    rows_dev, members = x_ref.shape
    n = var_ref.shape[1]
    ncols = kept_ref.shape[0]
    per_dev = n // ncols
    groups = per_dev // 8
    chunks = members // 128
    core = lax.axis_index("row") & 1
    scale = 1.0 / (members - 1.0)
    obs1, obs0 = rows_dev, rows_dev + n

    def member_chunk(i, side):
        return pl.ds(pl.multiple_of((2 * i + (core if side == 0 else 1 - core)) * 128, 128), 128)

    def chunk(j, width):
        return pl.ds(pl.multiple_of(j * width, width), width)

    def observed(b, i, ref):
        return jnp.concatenate(
            [ref[(b * groups + g) * (chunks // 2) + i, c] for c in range(ncols) for g in range(groups)], axis=0
        )

    def add_up(c, carry):
        for b, top in ((0, obs0), (1, obs1)):
            for g in range(groups):
                slots = [(b * groups + g) * (chunks // 2) + i for i in range(chunks // 2)]
                total = own_ref[slots[0], c] + other_ref[slots[0], c]
                for slot in slots[1:]:
                    total = total + (own_ref[slot, c] + other_ref[slot, c])
                mean_ref[pl.ds(pl.multiple_of(top + c * per_dev + g * 8, 8), 8), :] = total
        return carry

    lax.fori_loop(0, ncols, add_up, 0, unroll=4)
    mean = jnp.sum(mean_ref[obs1:, :], axis=1, keepdims=True) * (1.0 / members)
    mean_ref[obs1:, :] = jnp.broadcast_to(mean, (2 * n, 128))
    mean_ref[:rows_dev, :] = x_mean_ref[...]

    wide = 2 * 128
    diag = lax.broadcasted_iota(jnp.int32, (n, n), 0) == lax.broadcasted_iota(jnp.int32, (n, n), 1)
    c_ref[...] = jnp.zeros_like(c_ref)

    def covariance0(i, carry):
        mean = mean_ref[obs0:, :]
        anom = jnp.concatenate([observed(0, i, own_ref) - mean, observed(0, i, other_ref) - mean], axis=1)
        parts = split(anom, 3)
        for p in range(3):
            s0_ref[p, :, chunk(i, wide)] = parts[p]
        c_ref[...] += dot_parts(parts, parts, 1)
        return carry

    lax.fori_loop(0, members // wide, covariance0, 0, unroll=4)
    for p, part in enumerate(split(c_ref[...], 3)):
        w_ref[p] = part
    c_ref[...] = c_ref[...] * scale + jnp.where(diag, var_ref[0:1, :], 0.0)
    t_ref[...] = jnp.zeros_like(t_ref)
    e_ref[...] = jnp.zeros_like(e_ref)

    def cross0(j):
        at, i, side = chunk(j, 128), j // 2, j % 2
        local = jnp.where(side == 0, x_ref[:, member_chunk(i, 0)], x_ref[:, member_chunk(i, 1)])
        seen = jnp.where(side == 0, observed(1, i, own_ref), observed(1, i, other_ref))
        anom = jnp.concatenate([local, seen - mean_ref[obs1:obs0, :]], axis=0)
        q_ref[:, at] = anom
        parts = split(anom, 3)
        t_ref[...] += dot_parts(parts, [s0_ref[p, :, at] for p in range(3)], 1)
        parts = [part[obs1:] for part in parts]
        e_ref[...] += dot_parts(parts, parts, 1)

    invert_in_place(c_ref, panel_ref, swept_ref, trans_ref, cross0)

    for p, part in enumerate(split(c_ref[...], 3)):
        v_ref[p] = part

    def gain(tapered, parts):
        return split(dot_parts(split(tapered, 3), [v_ref[p] for p in range(3)], 0), parts)

    for half in range(2):
        kept = jnp.concatenate(
            [
                jnp.concatenate(
                    [jnp.broadcast_to(kept_ref[c : c + 1, i : i + 1] * -scale, (per_dev, 128)) for i in range(2)],
                    axis=1,
                )
                for c in range(half * ncols // 2, (half + 1) * ncols // 2)
            ],
            axis=0,
        )
        rows = slice(half * n // 2, (half + 1) * n // 2)
        at = slice(obs1 + half * n // 2, obs1 + (half + 1) * n // 2)
        for p, part in enumerate(gain(t_ref[at, :] * (decay_ref[rows, :] * kept), 3)):
            g_ref[p, at, :] = part

    for half in range(2):
        at = slice(obs1 + half * n // 2, obs1 + (half + 1) * n // 2)
        product = dot_parts([g_ref[p, at, :] for p in range(3)], [w_ref[p] for p in range(3)], 0)
        for p, part in enumerate(split(0.25 * product - t_ref[at, :], 3)):
            v1_ref[p, half * n // 2 : (half + 1) * n // 2, :] = part
    for half in range(2):
        at = slice(obs1 + half * n // 2, obs1 + (half + 1) * n // 2)
        c_ref[half * n // 2 : (half + 1) * n // 2, :] = dot_parts(
            [g_ref[p, at, :] for p in range(3)], [v1_ref[p] for p in range(3)], 1
        )
    c_ref[...] = (e_ref[...] + 0.5 * (c_ref[...] + c_ref[...].T)) * scale + jnp.where(diag, var_ref[1:2, :], 0.0)

    for p, part in enumerate(gain(t_ref[:rows_dev, :] * (rho_ref[0] * -scale), 2)):
        g_ref[p, :rows_dev, :] = part
    for p, part in enumerate(split(value_ref[:, 0:1] - mean_ref[obs0:, :], 3)):
        innov_ref[p] = part
    t_ref[:rows_dev, :] = jnp.zeros((rows_dev, n), jnp.float32)

    def cross1(j):
        at = chunk(j, 128)
        some = pl.ds(pl.multiple_of(obs1 + j * (n // chunks), n // chunks), n // chunks)
        mean_ref[some, :] += dot_parts(
            [g_ref[p, some, :] for p in range(3)], [innov_ref[p] for p in range(3)], 0
        )
        some = chunk(j, rows_dev // chunks)
        mean_ref[some, :] += dot_parts(
            [g_ref[p, some, :] for p in range(2)], [innov_ref[p] for p in range(2)], 0
        )
        change = dot_parts(
            [g_ref[p, obs1:obs0, :] for p in range(3)], [s0_ref[p, :, at] for p in range(3)], 0
        )
        seen = split(q_ref[obs1:obs0, at] - 0.5 * change, 3)
        for p in range(3):
            s1_ref[p, :, at] = seen[p]
        change = dot_parts(
            [g_ref[p, :rows_dev, :] for p in range(2)], [s0_ref[p, :, at] for p in range(2)], 0
        )
        anom = q_ref[:rows_dev, at] - 0.5 * change
        q_ref[:rows_dev, at] = anom
        t_ref[:rows_dev, :] += dot_parts(split(anom, 3), seen, 1)

    invert_in_place(c_ref, panel_ref, swept_ref, trans_ref, cross1)
    innov1 = split(value_ref[:, 1:2] - mean_ref[obs1:obs0, :], 2)
    for p, part in enumerate(split(c_ref[...], 3)):
        v_ref[p] = part
    gain1 = gain(t_ref[:rows_dev, :] * (rho_ref[1] * -scale), 2)
    mean = mean_ref[:rows_dev, :] + dot_parts(gain1, innov1, 0)
    copies = []
    for i in range(members // wide):
        at = slice(i * wide, (i + 1) * wide)
        change = dot_parts(gain1, [s1_ref[p, :, at] for p in range(2)], 0)
        stage_ref[:, at] = jnp.concatenate([mean] * 2, axis=1) + q_ref[:rows_dev, at] - 0.5 * change
        for side in range(2):
            j = 2 * i + side
            copies.append(
                pltpu.make_async_copy(
                    stage_ref.at[:, 128 * j : 128 * j + 128], out_ref.at[:, member_chunk(i, side)], sems.at[j]
                )
            )
            copies[-1].start()
    for copy in copies:
        copy.wait()


def on_core(kernel, name, outs, smem, vmem, scratch=(), limit_mib=6):
    return pl.pallas_call(
        kernel,
        out_shape=outs,
        in_specs=[pl.BlockSpec(memory_space=SMEM)] * len(smem) + [pl.BlockSpec(memory_space=VMEM)] * len(vmem),
        out_specs=jax.tree.map(lambda _: pl.BlockSpec(memory_space=VMEM), outs),
        scratch_shapes=list(scratch),
        compiler_params=pltpu.CompilerParams(vmem_limit_bytes=limit_mib and limit_mib * 1024 * 1024),
        name=name,
    )(*smem, *vmem)


def exchange(x, axis, groups=None):
    return lax.all_to_all(x, axis, split_axis=0, concat_axis=0, axis_index_groups=groups, tiled=True)


def floats(*shape):
    return jax.ShapeDtypeStruct(shape, jnp.float32)


def prepare(owner, taper_mask, ensemble, obs_rows, obs_value, obs_var, ncols, local_len):
    rows_dev, members = ensemble.shape
    n = obs_rows.shape[1]
    return on_core(
        functools.partial(prepare_kernel, ncols=ncols, local_len=local_len), "prepare",
        (floats(2, rows_dev, n), floats(n, n), floats(rows_dev, members), floats(rows_dev, 128),
         floats(n, 128), floats(2, n)),
        (owner, taper_mask), (ensemble, obs_rows, obs_value, obs_var), limit_mib=None,
    )


def assimilate(own, other, kept, prepared):
    rows_dev, members = prepared[2].shape
    n = prepared[1].shape[0]
    total = rows_dev + 2 * n
    return pl.pallas_call(
        assimilate_kernel,
        out_shape=floats(rows_dev, members),
        in_specs=[pl.BlockSpec(memory_space=VMEM)] * (3 + len(prepared)),
        out_specs=pl.BlockSpec(memory_space=pl.ANY),
        scratch_shapes=[
            VMEM((rows_dev + n, members), jnp.float32),
            VMEM((3, n, members), jnp.bfloat16),
            VMEM((3, n, members), jnp.bfloat16),
            VMEM((rows_dev + n, n), jnp.float32),
            VMEM((n, n), jnp.float32),
            VMEM((3, rows_dev + n, n), jnp.bfloat16),
            VMEM((total, 128), jnp.float32),
            VMEM((PIVOTS, n), jnp.float32),
            VMEM((2, PIVOTS, n), jnp.float32),
            VMEM((2, n, len(TERMS) * PIVOTS), jnp.bfloat16),
            VMEM((3, n, n), jnp.bfloat16),
            VMEM((3, n, 128), jnp.bfloat16),
            VMEM((3, n, n), jnp.bfloat16),
            VMEM((3, n, n), jnp.bfloat16),
            VMEM((n, n), jnp.float32),
            VMEM((rows_dev, members), jnp.float32),
            pltpu.SemaphoreType.DMA((members // 128,)),
        ],
        compiler_params=pltpu.CompilerParams(vmem_limit_bytes=40 * 1024 * 1024),
        name="assimilate",
    )(own, other, kept, *prepared)


def on_device(ensemble, obs_rows, owner, obs_value, obs_var, taper_mask):
    rows, members = ensemble.shape
    ncols, nrows = lax.axis_size("col"), lax.axis_size("row")
    per_dev = obs_rows.shape[1] // ncols
    picked = on_core(
        pick_kernel, "pick_rows", floats(nrows, 1, 1024 + 128),
        (obs_rows, taper_mask), (ensemble,), [VMEM((2 * per_dev, members), jnp.float32)], None,
    )
    pieces = exchange(picked, "row")
    prepared = prepare(owner, taper_mask, ensemble, obs_rows, obs_value, obs_var, ncols, rows * nrows * ncols // 4)
    wanted = on_core(
        functools.partial(choose_kernel, nrows=nrows), "choose",
        jax.ShapeDtypeStruct((1, 1024 + 128), jnp.int32), (owner,), (),
    )
    pieces, wanted, *prepared = lax.optimization_barrier((pieces, wanted, *prepared))
    taken = jnp.arange(nrows, dtype=jnp.int32)[:, None, None] == wanted[None]
    line = jnp.sum(jnp.where(taken, pieces, 0.0), axis=0)
    line = jnp.broadcast_to(line[None], (ncols, 1, 1024 + 128))
    line = exchange(line, "col")
    wide, kept = on_core(
        share_kernel, "share", (floats(nrows // 2, ncols, 8, 128), floats(ncols, 128)),
        (), (line,), [VMEM((ncols, 8, 128), jnp.float32)],
    )
    own = exchange(wide, "row", [[r for r in range(nrows) if r % 2 == c] for c in range(2)])
    other = lax.ppermute(own, "row", [(r, r ^ 1) for r in range(nrows)])
    return assimilate(own, other, kept, prepared)


def solution(mesh):
    in_specs = (P(("row", "col"), None), P(), P(), P(), P(), P(None, ("row", "col"), None))
    out_specs = P(("row", "col"), None)
    return jax.shard_map(
        on_device, mesh=mesh, in_specs=in_specs, out_specs=out_specs, check_vma=False
    )
```
